256 devices in a mesh: rows: 64 (over z, x, core), rep: 4 (over y).
Axes of the slice: x: 4, y: 4, z: 8, core: 2. Of those that a mesh axis runs over, the one named last changes fastest.
Arguments:
- p_blocks: bfloat16 [512, 12, 128, 128], P('rows'), may hold values from -1.25 to 1.25
- d_blocks: bfloat16 [512, 12, 128, 128], P('rows'), may hold values from -1.25 to 1.25
- p_cols: int32 [512, 12], replicated, may hold values from 0 to 511, as said below
- d_cols: int32 [512, 12], replicated, may hold values from 0 to 511, as said below
- out_pcols: int32 [512, 12], P('rows'), may hold values from 0 to 511, as said below
- out_dcols: int32 [512, 12], P('rows'), may hold values from 0 to 511, as said below
- row_slot: int32 [512], replicated, may hold values from 0 to 511, as said below
- branch: int32 [512], P('rows'), may hold values from 0 to 1
Outputs:
- next_p: bfloat16 [512, 12, 128, 128], P('rows', 'rep')
- next_d: bfloat16 [512, 12, 128, 128], P('rows', 'rep')
The draws below stay inside these ranges and needn't reach their ends.
Inputs may be any that keep to these rules, and one draw needn't show every extreme that they name: row_slot is a permutation; global block row g is stored at position row_slot[g], on index row_slot[g] // 8 of rows, and never more than 3 positions away from g. `p_cols`: the stored row s that holds global block row g names 12 different global block columns, g among them, each equal to (g + o) mod 512 with -12 <= o <= 12. `d_cols`: as for p_cols. `out_pcols`: as for p_cols. `out_dcols`: as for p_cols.
All inputs are finite; a program needn't handle non-finite values.
Results may differ from the reference program's by a relative error of at most 0.0095.
Values may be sent and summed in bfloat16 or wider, within the bound.
No kernel may reach another device: no remote copies, remote signals or barrier semaphores. Data moves between devices by JAX's collectives and lax.ppermute only.
A program may use at most 192 MiB of HBM per device.

```python
import jax
import jax.numpy as jnp
from jax import lax

B = 128
K = 12
KQ = 3
NB = 512
SPREAD = 4


def storage_order(base_key):
    group_count = NB // SPREAD
    scores = jax.random.randint(jax.random.fold_in(base_key, 505), (group_count, SPREAD), 0, 1 << 20) * SPREAD + jnp.arange(SPREAD, dtype=jnp.int32)[None, :]
    local = jnp.argsort(scores, axis=1).astype(jnp.int32)
    order = jnp.arange(group_count, dtype=jnp.int32)[:, None] * SPREAD + local
    return order.reshape(NB).astype(jnp.int32)


def band_columns(base_key, salt_value):
    pattern_key = jax.random.fold_in(base_key, salt_value)
    key_pick, key_slots = jax.random.split(pattern_key)
    offsets = jnp.concatenate([jnp.arange(-K, 0), jnp.arange(1, K + 1)]).astype(jnp.int32)
    scores = jax.random.randint(key_pick, (NB, 2 * K), 0, 1 << 20) * (2 * K) + jnp.arange(2 * K, dtype=jnp.int32)[None, :]
    chosen = jnp.argsort(scores, axis=1)[:, :K - 1]
    global_ids = storage_order(base_key)[:, None]
    columns = jnp.concatenate([global_ids, (global_ids + offsets[chosen]) % NB], axis=1)
    slot_scores = jax.random.randint(key_slots, (NB, K), 0, 1 << 20) * K + jnp.arange(K, dtype=jnp.int32)[None, :]
    slot_order = jnp.argsort(slot_scores, axis=1)
    return jnp.take_along_axis(columns, slot_order, axis=1).astype(jnp.int32)


def draw_p_cols(key, part):
    return band_columns(key, 101)


def draw_d_cols(key, part):
    return band_columns(key, 202)


def draw_out_pcols(key, part):
    return band_columns(key, 303)


def draw_out_dcols(key, part):
    return band_columns(key, 404)


def draw_row_slot(key, part):
    return jnp.argsort(storage_order(key)).astype(jnp.int32)


def plant(result, stream_key, low, top_value):
    shape = result.shape
    place = [jax.random.randint(jax.random.fold_in(stream_key, axis), (), 0, shape[axis]) for axis in range(len(shape))]
    result = result.at[tuple(place)].set(low)
    longest = shape.index(max(shape))
    place[longest] = (place[longest] + 1) % shape[longest]
    return result.at[tuple(place)].set(top_value)


def level_of(rng, extent, cuts, low, high):
    gain, own = 1.0, jax.random.fold_in(rng, 6)
    for axis_at, blocks in cuts:
        draws = jnp.exp(jax.random.uniform(jax.random.fold_in(own, axis_at), (blocks,), jnp.float32, low / len(cuts), high / len(cuts)))
        gain = gain * jnp.repeat(draws, extent[axis_at] // blocks).reshape([-1 if axis == axis_at else 1 for axis in range(len(extent))])
    return gain


def scatter_about(key, dims, spread, limit, cuts=(), kind=jnp.bfloat16):
    values = spread * jax.random.normal(key, dims, jnp.float32)
    if cuts:
        values = values * level_of(key, dims, cuts, -0.22, 0.18)
    return jnp.clip(values, -limit, limit).astype(kind)


def setup_inputs(seed: int = 0) -> dict:
    arg_keys = jax.random.split(jax.random.key(seed), 9)
    p_blocks = scatter_about(arg_keys[0], (NB, K, B, B), 0.2, 1.25, ((0, 64),))
    d_blocks = scatter_about(arg_keys[1], (NB, K, B, B), 0.2, 1.25, ((0, 64),))
    p_cols = draw_p_cols(jax.random.fold_in(arg_keys[8], 71), 0)
    d_cols = draw_d_cols(jax.random.fold_in(arg_keys[8], 71), 0)
    out_pcols = draw_out_pcols(jax.random.fold_in(arg_keys[8], 71), 0)
    out_dcols = draw_out_dcols(jax.random.fold_in(arg_keys[8], 71), 0)
    row_slot = draw_row_slot(jax.random.fold_in(arg_keys[8], 71), 0)
    branch = plant(jax.random.randint(arg_keys[7], (NB,), 0, 2), jax.random.fold_in(arg_keys[7], 1), 0, 1).astype(jnp.int32)
    return dict(p_blocks=p_blocks, d_blocks=d_blocks, p_cols=p_cols, d_cols=d_cols, out_pcols=out_pcols, out_dcols=out_dcols, row_slot=row_slot, branch=branch)


def quarter_products(left_row, left_ids, out_row, right_blocks, right_cols, row_slot):
    stored = jnp.take(row_slot, left_ids, axis=0).astype(jnp.int32)
    right_rows = jnp.take(right_blocks, stored, axis=0).astype(jnp.float32)
    right_ids = jnp.take(right_cols, stored, axis=0)
    block_terms = jnp.einsum("kab,kmbc->kmac", left_row.astype(jnp.float32), right_rows, precision=lax.Precision.HIGHEST)
    matches = (right_ids[:, :, None] == out_row[None, None, :]).astype(jnp.float32)
    matches = matches.reshape(K, K // KQ, KQ, K)
    block_terms = block_terms.reshape(K, K // KQ, KQ, B, B)
    return jnp.einsum("kqmj,kqmac->qjac", matches, block_terms, precision=lax.Precision.HIGHEST)


def rounded_sum(quarter_parts):
    narrow = lax.optimization_barrier(quarter_parts.astype(jnp.bfloat16))
    return jnp.sum(narrow.astype(jnp.float32), axis=0)


def kept_blocks(row_blocks, row_ids, out_row):
    matches = (row_ids[:, None] == out_row[None, :]).astype(jnp.float32)
    return jnp.einsum("kj,kab->jab", matches, row_blocks.astype(jnp.float32), precision=lax.Precision.HIGHEST)


def reference(p_blocks, d_blocks, p_cols, d_cols, out_pcols, out_dcols, row_slot, branch):
    def one_row(row_items):
        p_row, d_row, p_ids, d_ids, p_out, d_out, row_bit = row_items
        squaring = row_bit == 1
        square = rounded_sum(quarter_products(p_row, p_ids, p_out, p_blocks, p_cols, row_slot))
        tangent = rounded_sum(quarter_products(p_row, p_ids, d_out, d_blocks, d_cols, row_slot) + quarter_products(d_row, d_ids, d_out, p_blocks, p_cols, row_slot))
        p_kept = kept_blocks(p_row, p_ids, p_out)
        d_kept = kept_blocks(d_row, d_ids, d_out)
        new_p = jnp.where(squaring, square, 2.0 * p_kept - square).astype(jnp.bfloat16)
        new_d = jnp.where(squaring, tangent, 2.0 * d_kept - tangent).astype(jnp.bfloat16)
        return new_p, new_d

    next_p, next_d = lax.map(one_row, (p_blocks, d_blocks, p_cols, d_cols, out_pcols, out_dcols, branch))
    return next_p, next_d
```

```python
import functools

import jax
import jax.numpy as jnp
from jax import lax
from jax.experimental import pallas as pl
from jax.experimental.pallas import tpu as pltpu
from jax.sharding import PartitionSpec as P

SPREAD_ROWS = 3
GROUP = 8


def shifted(value, axis, steps):
    count = lax.axis_size(axis)
    pairs = [(source, (source + steps) % count) for source in range(count)]
    return lax.ppermute(value, axis, pairs)


def neighbour_rows(part, slab_rows, margin_rows):
    lower, upper = [], []
    low = up = part
    left = margin_rows
    while left > 0:
        take = min(slab_rows, left)
        low = shifted(low[slab_rows - take :], "rows", 1)
        up = shifted(up[:take], "rows", -1)
        lower.append(low)
        upper.append(up)
        left -= take
    return lower[::-1] + [part] + upper


def match_list(code, valid, dump):
    rows, length = code.shape
    padded = -(-length // GROUP) * GROUP
    before = jnp.arange(length)[:, None] < jnp.arange(length)[None, :]
    rank = jnp.sum(jnp.where(before[None] & valid[:, :, None], 1, 0), axis=1)
    place = jnp.where(valid, rank, padded)
    hit = place[:, :, None] == jnp.arange(padded)[None, None, :]
    listed = jnp.sum(jnp.where(hit, code[:, :, None] - dump, 0), axis=1) + dump
    return listed.reshape(-1).astype(jnp.int32), jnp.sum(valid, axis=1).astype(jnp.int32)


def product_kernel(spans, quarters, count_ref, list_ref, *refs):
    n_left = len(spans)
    left_refs = refs[:n_left]
    piece_refs = refs[n_left : n_left + sum(len(span) for span in spans)]
    out_ref, window_ref, total_ref, sems = refs[-4:]
    row = pl.program_id(0)
    slots = left_refs[0].shape[1]
    padded = list_ref.shape[0] // count_ref.shape[0]

    copies = []
    base, index = 0, 0
    for span in spans:
        for rows in span:
            copies.append(
                pltpu.make_async_copy(
                    piece_refs[index], window_ref.at[pl.ds(base, rows)], sems.at[index]
                )
            )
            base += rows
            index += 1

    @pl.when(row == 0)
    def _():
        for copy in copies:
            copy.start()
        for copy in copies:
            copy.wait()

    total_ref[...] = jnp.zeros_like(total_ref)

    def step(group, carry):
        for u in range(GROUP):
            code = list_ref[row * padded + group * GROUP + u]
            target = code & 15
            slot = (code >> 4) & 3
            place = (code >> 6) & 127
            k = code >> 13
            if n_left == 1:
                left = left_refs[0][0, k]
            else:
                second = k >= slots
                kk = jnp.where(second, k - slots, k)
                left = jnp.where(second, left_refs[1][0, kk], left_refs[0][0, kk])
            total_ref[target] += jnp.dot(
                left, window_ref[place, slot], preferred_element_type=jnp.float32
            )
        return carry

    groups = (count_ref[row] + GROUP - 1) // GROUP
    lax.fori_loop(0, groups, step, 0)
    per = slots // quarters
    for j in range(slots):
        out_ref[j // per, 0, j % per] = total_ref[j].astype(out_ref.dtype)


def block_products(lefts, windows, listed, counts, quarters):
    slab_rows, slots, side, _ = lefts[0].shape
    per = slots // quarters
    spans = tuple(tuple(piece.shape[0] for piece in window) for window in windows)
    pieces = [piece for window in windows for piece in window]
    rows_in = sum(sum(span) for span in spans)
    flops = 2 * side**3 * listed.shape[0] // 2
    any_spec = pl.BlockSpec(memory_space=pl.ANY)
    return pl.pallas_call(
        functools.partial(product_kernel, spans, quarters),
        grid_spec=pltpu.PrefetchScalarGridSpec(
            num_scalar_prefetch=2,
            grid=(slab_rows,),
            in_specs=[pl.BlockSpec((1, slots, side, side), lambda s, *_: (s, 0, 0, 0))] * len(lefts)
            + [any_spec] * len(pieces),
            out_specs=pl.BlockSpec((quarters, 1, per, side, side), lambda s, *_: (0, s, 0, 0, 0)),
            scratch_shapes=[
                pltpu.VMEM((rows_in, per, side, side), lefts[0].dtype),
                pltpu.VMEM((slots + 1, side, side), jnp.float32),
                pltpu.SemaphoreType.DMA((len(pieces),)),
            ],
        ),
        out_shape=jax.ShapeDtypeStruct((quarters, slab_rows, per, side, side), jnp.bfloat16),
        compiler_params=pltpu.CompilerParams(
            dimension_semantics=("arbitrary",), vmem_limit_bytes=32 << 20
        ),
        cost_estimate=pl.CostEstimate(
            flops=flops, bytes_accessed=2 * (rows_in * per + 2 * slab_rows * slots) * side * side,
            transcendentals=0,
        ),
        name="block_products",
    )(counts, listed, *lefts, *pieces)


def finish_kernel(branch_ref, kept_ref, parts_ref, row_ref, out_ref):
    row = pl.program_id(0)
    slots = row_ref.shape[1]
    per = out_ref.shape[1]
    squaring = branch_ref[row] == 1
    for j in range(per):
        total = parts_ref[0, 0, j].astype(jnp.float32)
        for q in range(1, parts_ref.shape[0]):
            total = total + parts_ref[q, 0, j].astype(jnp.float32)
        place = kept_ref[row * per + j]
        kept = row_ref[0, jnp.minimum(place, slots - 1)].astype(jnp.float32)
        kept = jnp.where(place < slots, kept, 0.0)
        out_ref[0, j] = jnp.where(squaring, total, 2.0 * kept - total).astype(out_ref.dtype)


def finish(parts, row_blocks, kept, branch):
    quarters, slab_rows, per, side, _ = parts.shape
    slots = row_blocks.shape[1]
    return pl.pallas_call(
        finish_kernel,
        grid_spec=pltpu.PrefetchScalarGridSpec(
            num_scalar_prefetch=2,
            grid=(slab_rows,),
            in_specs=[
                pl.BlockSpec((quarters, 1, per, side, side), lambda s, *_: (0, s, 0, 0, 0)),
                pl.BlockSpec((1, slots, side, side), lambda s, *_: (s, 0, 0, 0)),
            ],
            out_specs=pl.BlockSpec((1, per, side, side), lambda s, *_: (s, 0, 0, 0)),
        ),
        out_shape=jax.ShapeDtypeStruct((slab_rows, per, side, side), jnp.bfloat16),
        compiler_params=pltpu.CompilerParams(
            dimension_semantics=("arbitrary",), vmem_limit_bytes=32 << 20
        ),
        name="finish",
    )(branch, kept, parts, row_blocks)


def local(p_blocks, d_blocks, p_cols, d_cols, out_pcols, out_dcols, row_slot, branch):
    slab_rows, slots, side, _ = p_blocks.shape
    quarters = lax.axis_size("rep")
    per = slots // quarters
    all_rows = p_cols.shape[0]
    row_start = lax.axis_index("rows") * slab_rows
    slot_start = lax.axis_index("rep") * per
    margin_rows = slots + 2 * SPREAD_ROWS
    window_rows = slab_rows + 2 * margin_rows

    p_part = lax.dynamic_slice_in_dim(p_blocks, slot_start, per, 1)
    d_part = lax.dynamic_slice_in_dim(d_blocks, slot_start, per, 1)
    p_window = neighbour_rows(p_part, slab_rows, margin_rows)
    d_window = neighbour_rows(d_part, slab_rows, margin_rows)

    own = jnp.stack(
        [
            lax.dynamic_slice_in_dim(p_cols, row_start, slab_rows, 0),
            lax.dynamic_slice_in_dim(d_cols, row_start, slab_rows, 0),
        ]
    )
    stored = jnp.take(row_slot, own, axis=0)
    place = (stored - row_start + margin_rows) % all_rows
    right = jnp.concatenate(
        [
            lax.dynamic_slice_in_dim(p_cols, slot_start, per, 1),
            lax.dynamic_slice_in_dim(d_cols, slot_start, per, 1),
        ],
        axis=1,
    )
    right_ids = jnp.take(right, stored, axis=0)

    def coded(left, right_ids, out_ids, k_base, place_base):
        matches = right_ids[:, :, :, None] == out_ids[:, None, None, :]
        valid = jnp.any(matches, axis=3)
        target = jnp.sum(jnp.where(matches, jnp.arange(slots), 0), axis=3)
        where_in = place[left][:, :, None] + place_base
        k = jnp.arange(slots)[None, :, None] + k_base
        code = target + (jnp.arange(per)[None, None, :] << 4) + (where_in << 6) + (k << 13)
        return code.reshape(slab_rows, -1), valid.reshape(slab_rows, -1)

    square_code = coded(0, right_ids[0, :, :, :per], out_pcols, 0, 0)
    pd = coded(0, right_ids[0, :, :, per:], out_dcols, 0, window_rows)
    dp = coded(1, right_ids[1, :, :, :per], out_dcols, slots, 0)
    tangent_code = tuple(jnp.concatenate(pair, axis=1) for pair in zip(pd, dp))
    square_list = match_list(*square_code, slots)
    tangent_list = match_list(*tangent_code, slots)

    square = block_products((p_blocks,), (p_window,), *square_list, quarters)
    square = lax.all_to_all(square, "rep", split_axis=0, concat_axis=0, tiled=True)
    tangent = block_products((p_blocks, d_blocks), (p_window, d_window), *tangent_list, quarters)
    tangent = lax.all_to_all(tangent, "rep", split_axis=0, concat_axis=0, tiled=True)

    def kept_place(own_ids, out_ids):
        out_quarter = lax.dynamic_slice_in_dim(out_ids, slot_start, per, 1)
        matches = own_ids[:, :, None] == out_quarter[:, None, :]
        position = jnp.sum(jnp.where(matches, jnp.arange(slots)[None, :, None], 0), axis=1)
        return jnp.where(jnp.any(matches, axis=1), position, slots).reshape(-1).astype(jnp.int32)

    next_p = finish(square, p_blocks, kept_place(own[0], out_pcols), branch)
    next_d = finish(tangent, d_blocks, kept_place(own[1], out_dcols), branch)
    return next_p, next_d


def solution(mesh):
    return jax.shard_map(
        local,
        mesh=mesh,
        in_specs=(
            P("rows", None, None, None),
            P("rows", None, None, None),
            P(),
            P(),
            P("rows", None),
            P("rows", None),
            P(),
            P("rows"),
        ),
        out_specs=(P("rows", "rep", None, None), P("rows", "rep", None, None)),
        check_vma=False,
    )
```

```python
import functools

import jax
import jax.numpy as jnp
import numpy as np
from jax import lax
from jax.experimental import pallas as pl
from jax.experimental.pallas import tpu as pltpu
from jax.sharding import PartitionSpec as P


SPREAD_ROWS = 3
GROUP = 8
VMEM_LIMIT = 67_000_000


def window_table(slab, margin):
    far = margin - 2 * slab
    sizes = (slab, slab, slab, slab - far, far, far, slab, far)
    own, in1, out1, near2, far2, out3, in2, in3 = np.cumsum((0,) + sizes[:-1])

    def run(start, count):
        return list(range(start, start + count))

    core0 = (
        run(out3, far) + run(near2, slab - far) + run(far2, far) + run(out1, slab)
        + run(own, slab) + run(in1, slab) + run(in2, slab) + run(in3, far)
    )
    core1 = (
        run(in3, far) + run(in2, slab) + run(in1, slab) + run(own, slab)
        + run(out1, slab) + run(far2, far) + run(near2, slab - far) + run(out3, far)
    )
    return sizes, np.array(core0 + core1, np.int32)


def swapped(value, even_step, odd_step):
    count = lax.axis_size("rows")
    pairs = [(i, (i + (odd_step if i % 2 else even_step)) % count) for i in range(count)]
    return lax.ppermute(value, "rows", pairs)


def pack_kernel(far, place_ref, blocks_ref, part_ref, near_ref, far_ref, edge_ref, held, sems):
    slab, per = held.shape[:2]
    core, rep = place_ref[0] % 2, place_ref[1]
    load = pltpu.make_async_copy(blocks_ref.at[:, pl.ds(rep * per, per)], held, sems.at[0])
    load.start()
    load.wait()
    rest = slab - far
    stores = [
        pltpu.make_async_copy(held, part_ref, sems.at[1]),
        pltpu.make_async_copy(held.at[pl.ds(core * far, rest)], near_ref, sems.at[2]),
        pltpu.make_async_copy(held.at[pl.ds((1 - core) * rest, far)], far_ref, sems.at[3]),
        pltpu.make_async_copy(held.at[pl.ds(core * rest, far)], edge_ref, sems.at[4]),
    ]
    for store in stores:
        store.start()
    for store in stores:
        store.wait()


def packed(blocks, place, per, far):
    slab, _, side, _ = blocks.shape
    shapes = [(slab, per), (slab - far, per), (far, per), (far, per)]
    return pl.pallas_call(
        functools.partial(pack_kernel, far),
        in_specs=[pl.BlockSpec(memory_space=pltpu.SMEM), pl.BlockSpec(memory_space=pl.ANY)],
        out_specs=[pl.BlockSpec(memory_space=pl.ANY)] * 4,
        out_shape=[jax.ShapeDtypeStruct(s + (side, side), blocks.dtype) for s in shapes],
        scratch_shapes=[
            pltpu.VMEM((slab, per, side, side), blocks.dtype),
            pltpu.SemaphoreType.DMA((5,)),
        ],
        compiler_params=pltpu.CompilerParams(vmem_limit_bytes=VMEM_LIMIT),
        cost_estimate=pl.CostEstimate(
            flops=2_000_000_000, bytes_accessed=2 * slab * per * side * side, transcendentals=0
        ),
        name="pack",
    )(place, blocks)


class Meta:
    def __init__(self, slab, slots, per):
        self.slab, self.slots, self.per = slab, slots, per
        self.square_pitch = slots * per + GROUP
        self.tangent_pitch = 2 * slots * per + GROUP
        self.square_count = 0
        self.tangent_count = slab
        self.kept = 2 * slab
        self.square = self.kept + 2 * slab * per
        self.tangent = self.square + slab * self.square_pitch
        self.size = self.tangent + slab * self.tangent_pitch


def plan_kernel(
    lay, margin, window_rows,
    place_ref, table_ref, pcols, dcols, opcols, odcols, row_slot, meta, inv_p, inv_d, inv_k,
):
    slab, slots, per = lay.slab, lay.slots, lay.per
    rows = row_slot.shape[0]
    index, rep = place_ref[0], place_ref[1]
    row_start = index * slab
    table_base = (index % 2) * window_rows

    def clear(step, carry):
        for u in range(16):
            for inv in (inv_p, inv_d, inv_k):
                inv[step * 16 + u] = slots
        return carry

    lax.fori_loop(0, rows // 16, clear, 0)

    def row(s, carry):
        out_base = s * slots
        own_base = (row_start + s) * slots
        for j in range(slots):
            inv_p[opcols[out_base + j]] = j
            inv_d[odcols[out_base + j]] = j
        square_at = lay.square + s * lay.square_pitch
        tangent_at = lay.tangent + s * lay.tangent_pitch
        square_start, tangent_start = square_at, tangent_at

        def located(column):
            stored = row_slot[column]
            offset = (stored - row_start + margin + rows) & (rows - 1)
            return table_ref[table_base + offset] * per, stored * slots + rep * per

        for k in range(slots):
            here, ids = located(pcols[own_base + k])
            for m in range(per):
                target = inv_p[pcols[ids + m]]
                meta[square_at] = target + ((here + m) << 4) + (k << 13)
                square_at += jnp.where(target < slots, 1, 0)
                target = inv_d[dcols[ids + m]]
                meta[tangent_at] = target + ((here + window_rows * per + m) << 4) + (k << 13)
                tangent_at += jnp.where(target < slots, 1, 0)
            here, ids = located(dcols[own_base + k])
            for m in range(per):
                target = inv_d[pcols[ids + m]]
                meta[tangent_at] = target + ((here + m) << 4) + ((k + slots) << 13)
                tangent_at += jnp.where(target < slots, 1, 0)
        for u in range(GROUP):
            meta[square_at + u] = slots
            meta[tangent_at + u] = slots
        meta[lay.square_count + s] = square_at - square_start
        meta[lay.tangent_count + s] = tangent_at - tangent_start
        for j in range(slots):
            inv_p[opcols[out_base + j]] = slots
            inv_d[odcols[out_base + j]] = slots

        for which, (cols, outs) in enumerate(((pcols, opcols), (dcols, odcols))):
            for k in range(slots):
                inv_k[cols[own_base + k]] = k
            for j in range(per):
                at = lay.kept + (which * slab + s) * per + j
                meta[at] = inv_k[outs[out_base + rep * per + j]]
            for k in range(slots):
                inv_k[cols[own_base + k]] = slots
        return carry

    lax.fori_loop(0, slab, row, 0)


def planned(lay, margin, window_rows, table, place, p_cols, d_cols, out_pcols, out_dcols, row_slot):
    rows = row_slot.shape[0]
    smem = pl.BlockSpec(memory_space=pltpu.SMEM)
    return pl.pallas_call(
        functools.partial(plan_kernel, lay, margin, window_rows),
        in_specs=[smem] * 7,
        out_specs=smem,
        out_shape=jax.ShapeDtypeStruct((lay.size,), jnp.int32),
        scratch_shapes=[pltpu.SMEM((rows,), jnp.int32)] * 3,
        compiler_params=pltpu.CompilerParams(vmem_limit_bytes=VMEM_LIMIT),
        cost_estimate=pl.CostEstimate(flops=6_000_000_000, bytes_accessed=65536, transcendentals=0),
        name="plan",
    )(
        place, jnp.asarray(table), p_cols.reshape(-1), d_cols.reshape(-1),
        out_pcols.reshape(-1), out_dcols.reshape(-1), row_slot,
    )


def kept_kernel(lay, meta, p_ref, d_ref, out_ref, held, sems, out_sem):
    slab, slots, per = lay.slab, lay.slots, lay.per
    loads = []
    for which, blocks in enumerate((p_ref, d_ref)):
        for s in range(slab):
            for j in range(per):
                n = (which * slab + s) * per + j
                k = meta[lay.kept + n]
                load = pltpu.make_async_copy(
                    blocks.at[s, jnp.minimum(k, slots - 1)], held.at[which, s, j], sems.at[n]
                )
                load.start()
                loads.append((load, k, which, s, j))
    for load, k, which, s, j in loads:
        load.wait()

        @pl.when(k == slots)
        def _():
            held[which, s, j] = jnp.zeros(held.shape[3:], held.dtype)

    store = pltpu.make_async_copy(held, out_ref, out_sem)
    store.start()
    store.wait()


def kept_blocks(lay, meta, p_blocks, d_blocks):
    slab, _, side, _ = p_blocks.shape
    shape = (2, slab, lay.per, side, side)
    return pl.pallas_call(
        functools.partial(kept_kernel, lay),
        in_specs=[pl.BlockSpec(memory_space=pltpu.SMEM)] + [pl.BlockSpec(memory_space=pl.ANY)] * 2,
        out_specs=pl.BlockSpec(memory_space=pl.ANY),
        out_shape=jax.ShapeDtypeStruct(shape, p_blocks.dtype),
        scratch_shapes=[
            pltpu.VMEM(shape, p_blocks.dtype),
            pltpu.SemaphoreType.DMA((2 * slab * lay.per,)),
            pltpu.SemaphoreType.DMA,
        ],
        compiler_params=pltpu.CompilerParams(vmem_limit_bytes=VMEM_LIMIT),
        cost_estimate=pl.CostEstimate(flops=3_000_000_000, bytes_accessed=1 << 21, transcendentals=0),
        name="kept",
    )(meta, p_blocks, d_blocks)


def product_kernel(n_left, sizes, count_at, list_at, pitch, quarters, meta, *refs):
    left_refs = refs[:n_left]
    pieces = refs[n_left : n_left + n_left * len(sizes)]
    out_ref, left, window, total, left_sems, sems = refs[-6:]
    row = pl.program_id(0)
    slab, slots = left_refs[0].shape[:2]
    per = slots // quarters

    def left_copy(s, n):
        return pltpu.make_async_copy(
            left_refs[n].at[s], left.at[s, pl.ds(n * slots, slots)], left_sems.at[s, n]
        )

    @pl.when(row == 0)
    def _():
        copies, base = [], 0
        for index, piece in enumerate(pieces):
            size = sizes[index % len(sizes)]
            copies.append(
                pltpu.make_async_copy(
                    piece, window.at[pl.ds(base * per, size * per)], sems.at[index]
                )
            )
            base += size
        for copy in copies:
            copy.start()
        for s in range(slab):
            for n in range(n_left):
                left_copy(s, n).start()
        for copy in copies:
            copy.wait()

    for n in range(n_left):
        left_copy(row, n).wait()
    total[...] = jnp.zeros_like(total)

    def step(group, carry):
        for u in range(GROUP):
            code = meta[list_at + row * pitch + group * GROUP + u]
            target = code & 15
            total[target] += jnp.dot(
                left[row, code >> 13], window[(code >> 4) & 511],
                preferred_element_type=jnp.float32,
            )
        return carry

    groups = (meta[count_at + row] + GROUP - 1) // GROUP
    lax.fori_loop(0, groups, step, 0)
    for j in range(slots):
        out_ref[j // per, 0, j % per] = total[j].astype(out_ref.dtype)


def block_products(lay, lefts, windows, sizes, meta, tangent, quarters):
    slab, slots, side, _ = lefts[0].shape
    per = lay.per
    pieces = [piece.reshape(-1, side, side) for window in windows for piece in window]
    rows_in = len(windows) * sum(sizes)
    dtype = lefts[0].dtype
    where = (
        (lay.tangent_count, lay.tangent, lay.tangent_pitch)
        if tangent
        else (lay.square_count, lay.square, lay.square_pitch)
    )
    any_spec = pl.BlockSpec(memory_space=pl.ANY)
    return pl.pallas_call(
        functools.partial(product_kernel, len(lefts), sizes, *where, quarters),
        grid_spec=pltpu.PrefetchScalarGridSpec(
            num_scalar_prefetch=1,
            grid=(slab,),
            in_specs=[any_spec] * (len(lefts) + len(pieces)),
            out_specs=pl.BlockSpec((quarters, 1, per, side, side), lambda s, *_: (0, s, 0, 0, 0)),
            scratch_shapes=[
                pltpu.VMEM((slab, len(lefts) * slots, side, side), dtype),
                pltpu.VMEM((rows_in * per, side, side), dtype),
                pltpu.VMEM((slots + 1, side, side), jnp.float32),
                pltpu.SemaphoreType.DMA((slab, len(lefts))),
                pltpu.SemaphoreType.DMA((len(pieces),)),
            ],
        ),
        out_shape=jax.ShapeDtypeStruct((quarters, slab, per, side, side), jnp.bfloat16),
        compiler_params=pltpu.CompilerParams(
            dimension_semantics=("arbitrary",), vmem_limit_bytes=VMEM_LIMIT
        ),
        cost_estimate=pl.CostEstimate(
            flops=12_000_000_000 if tangent else 8_000_000_000,
            bytes_accessed=2 * (rows_in * per + 2 * slab * slots) * side * side,
            transcendentals=0,
        ),
        name="tangent_products" if tangent else "square_products",
    )(meta, *lefts, *pieces)


def finish_kernel(rows, branch_ref, parts_ref, kept_ref, out_ref):
    step = pl.program_id(0)
    for s in range(rows):
        squaring = branch_ref[step * rows + s] == 1
        total = parts_ref[0, s].astype(jnp.float32)
        for q in range(1, parts_ref.shape[0]):
            total = total + parts_ref[q, s].astype(jnp.float32)
        kept = kept_ref[0, s].astype(jnp.float32)
        out_ref[s] = jnp.where(squaring, total, 2.0 * kept - total).astype(out_ref.dtype)


def finish(parts, kept, which, branch):
    quarters, slab, per, side, _ = parts.shape
    rows = 2
    return pl.pallas_call(
        functools.partial(finish_kernel, rows),
        grid_spec=pltpu.PrefetchScalarGridSpec(
            num_scalar_prefetch=1,
            grid=(slab // rows,),
            in_specs=[
                pl.BlockSpec((quarters, rows, per, side, side), lambda s, *_: (0, s, 0, 0, 0)),
                pl.BlockSpec((1, rows, per, side, side), lambda s, *_: (which, s, 0, 0, 0)),
            ],
            out_specs=pl.BlockSpec((rows, per, side, side), lambda s, *_: (s, 0, 0, 0)),
        ),
        out_shape=jax.ShapeDtypeStruct((slab, per, side, side), jnp.bfloat16),
        compiler_params=pltpu.CompilerParams(
            dimension_semantics=("arbitrary",), vmem_limit_bytes=VMEM_LIMIT
        ),
        cost_estimate=pl.CostEstimate(flops=4_000_000_000, bytes_accessed=5 << 20, transcendentals=0),
        name="finish",
    )(branch, parts, kept)


def step(p_blocks, d_blocks, p_cols, d_cols, out_pcols, out_dcols, row_slot, branch):
    slab, slots, _, _ = p_blocks.shape
    quarters = lax.axis_size("rep")
    per = slots // quarters
    margin = slots + 2 * SPREAD_ROWS
    far = margin - 2 * slab
    sizes, table = window_table(slab, margin)
    lay = Meta(slab, slots, per)
    place = jnp.stack([lax.axis_index("rows"), lax.axis_index("rep")]).astype(jnp.int32)

    def outer(blocks, place):
        part, near, rest, edge = packed(blocks, place, per, far)
        out1 = swapped(part, -1, 1)
        far2 = swapped(rest, 2, -2)
        near2 = swapped(near, 2, -2)
        out3 = swapped(edge, -3, 3)
        in1 = swapped(part, 1, -1)
        return part, in1, out1, near2, far2, out3

    def inner(pieces):
        return pieces + (swapped(pieces[2], 1, -1), swapped(pieces[4], 1, -1))

    p_window = outer(p_blocks, place)
    d_place, p_part = lax.optimization_barrier((place, p_window[0]))
    p_window = (p_part,) + p_window[1:]
    d_window = outer(d_blocks, d_place)
    meta = planned(
        lay, margin, sum(sizes), table, d_place, p_cols, d_cols, out_pcols, out_dcols, row_slot
    )
    p_window = inner(p_window)
    d_window = inner(d_window)
    square = block_products(lay, (p_blocks,), (p_window,), sizes, meta, False, quarters)
    square, kept_meta = lax.optimization_barrier((square, meta))
    square = lax.all_to_all(square, "rep", split_axis=0, concat_axis=0, tiled=True)
    kept = kept_blocks(lay, kept_meta, p_blocks, d_blocks)
    kept, tangent_meta = lax.optimization_barrier((kept, kept_meta))
    tangent = block_products(
        lay, (p_blocks, d_blocks), (p_window, d_window), sizes, tangent_meta, True, quarters
    )
    tangent, square = lax.optimization_barrier((tangent, square))
    tangent = lax.all_to_all(tangent, "rep", split_axis=0, concat_axis=0, tiled=True)
    return finish(square, kept, 0, branch), finish(tangent, kept, 1, branch)


def solution(mesh):
    return jax.shard_map(
        step,
        mesh=mesh,
        in_specs=(
            P("rows", None, None, None),
            P("rows", None, None, None),
            P(),
            P(),
            P("rows", None),
            P("rows", None),
            P(),
            P("rows"),
        ),
        out_specs=(P("rows", "rep", None, None), P("rows", "rep", None, None)),
        check_vma=False,
    )
```

```python
import functools

import jax
import jax.numpy as jnp
import numpy as np
from jax import lax
from jax.experimental import pallas as pl
from jax.experimental.pallas import tpu as pltpu
from jax.sharding import PartitionSpec as P


SPREAD_ROWS = 3
GROUP = 8
VMEM_LIMIT = 67_000_000


def window_table(slab, margin):
    far = margin - 2 * slab
    sizes = (slab, slab, slab, slab - far, far, far, slab, far)
    own, in1, out1, near2, far2, out3, in2, in3 = np.cumsum((0,) + sizes[:-1])

    def run(start, count):
        return list(range(start, start + count))

    core0 = (
        run(out3, far) + run(near2, slab - far) + run(far2, far) + run(out1, slab)
        + run(own, slab) + run(in1, slab) + run(in2, slab) + run(in3, far)
    )
    core1 = (
        run(in3, far) + run(in2, slab) + run(in1, slab) + run(own, slab)
        + run(out1, slab) + run(far2, far) + run(near2, slab - far) + run(out3, far)
    )
    edge = [0] * (slab - far)
    return sizes, np.array(edge + core0 + edge + edge + core1 + edge, np.int32)


def swapped(value, even_step, odd_step):
    count = lax.axis_size("rows")
    pairs = [(i, (i + (odd_step if i % 2 else even_step)) % count) for i in range(count)]
    return lax.ppermute(value, "rows", pairs)


def pack_kernel(far, *refs):
    blocks, outs, (held, sems) = refs[:2], refs[2:10], refs[10:]
    slab, per = held.shape[1:3]
    core, rep = lax.axis_index("rows") % 2, lax.axis_index("rep")
    rest = slab - far
    loads = [
        pltpu.make_async_copy(block.at[:, pl.ds(rep * per, per)], held.at[n], sems.at[n, 4])
        for n, block in enumerate(blocks)
    ]
    for load in loads:
        load.start()
    stores = []
    for n, load in enumerate(loads):
        load.wait()
        cuts = (
            held.at[n],
            held.at[n, pl.ds(core * far, rest)],
            held.at[n, pl.ds((1 - core) * rest, far)],
            held.at[n, pl.ds(core * rest, far)],
        )
        for i, cut in enumerate(cuts):
            store = pltpu.make_async_copy(cut, outs[4 * n + i], sems.at[n, i])
            store.start()
            stores.append(store)
    for store in stores:
        store.wait()


def packed(p_blocks, d_blocks, per, far):
    slab, _, side, _ = p_blocks.shape
    dtype = p_blocks.dtype
    shapes = [(slab, per), (slab - far, per), (far, per), (far, per)] * 2
    outs = pl.pallas_call(
        functools.partial(pack_kernel, far),
        in_specs=[pl.BlockSpec(memory_space=pl.ANY)] * 2,
        out_specs=[pl.BlockSpec(memory_space=pl.ANY)] * 8,
        out_shape=[jax.ShapeDtypeStruct(s + (side, side), dtype) for s in shapes],
        scratch_shapes=[
            pltpu.VMEM((2, slab, per, side, side), dtype),
            pltpu.SemaphoreType.DMA((2, 5)),
        ],
        compiler_params=pltpu.CompilerParams(vmem_limit_bytes=VMEM_LIMIT),
        cost_estimate=pl.CostEstimate(flops=3_000_000_000, bytes_accessed=1 << 22, transcendentals=0),
        name="pack",
    )(p_blocks, d_blocks)
    return outs[:4], outs[4:]


class Lists:
    def __init__(self, slab, slots, per, n_lists, kept):
        self.slab, self.slots, self.per, self.n_lists = slab, slots, per, n_lists
        self.pitch = slots * per + GROUP
        self.counts = [n * slab for n in range(n_lists)]
        self.kept = n_lists * slab if kept else None
        base = n_lists * slab + (2 * slab * per if kept else 0)
        self.lists = [base + n * slab * self.pitch for n in range(n_lists)]
        self.size = base + n_lists * slab * self.pitch


def plan_kernel(lay, reach, window_rows, products, table, row_slot, *refs):
    n = 1 + max(max(product) for product in products)
    cols_hbm, outs = refs[:n], refs[n : 2 * n]
    meta = refs[2 * n]
    cols, inverse, (slot_of, sems) = refs[2 * n + 1 : 3 * n + 1], refs[3 * n + 1 : 4 * n + 1], refs[-2:]
    slab, slots, per = lay.slab, lay.slots, lay.per
    rows = row_slot.shape[0]
    index, rep = lax.axis_index("rows"), lax.axis_index("rep")
    row_start = index * slab
    slabs = rows // slab
    width = 2 * reach + 1
    table_base = (index % 2) * (width * slab)

    copies = []
    for which in range(n):
        for near in range(width):
            at = (index + near + slabs - reach) & (slabs - 1)
            copies.append(
                pltpu.make_async_copy(
                    cols_hbm[which].at[pl.ds(at * slab, slab)],
                    cols[which].at[pl.ds(near * slab, slab)],
                    sems.at[which * width + near],
                )
            )
    for copy in copies:
        copy.start()
    span = 2 * slots + SPREAD_ROWS
    for column in range(-span, slab + span):
        for inv in inverse + ((slot_of,) if lay.kept is not None else ()):
            inv[(row_start + column + rows) & (rows - 1)] = slots
    for copy in copies:
        copy.wait()
    relative = [(q ^ rep) * per for q in range(slots // per)]
    here = reach * slab

    def row(s, carry):
        for which in range(n):
            for j in range(slots):
                inverse[which][outs[which][s, j]] = relative[j // per] + j % per
        starts = [base + s * lay.pitch for base in lay.lists]
        ends = list(starts)
        lefts = sorted({product[0] for product in products})
        for k in range(slots):
            for left in lefts:
                offset = (row_slot[cols[left][here + s, k]] - row_start + here + rows) & (rows - 1)
                place = table[table_base + offset]
                code = (place << 4) + (k << 13)
                found = []
                for number, (which_left, right, out) in enumerate(products):
                    if which_left != left:
                        continue
                    for m in range(per):
                        target = inverse[out][cols[right][offset, rep * per + m]]
                        shift = (right if n > 1 else 0) * window_rows * per + m
                        found.append((number, target, code + (shift << 4) + target))
                for number, target, entry in found:
                    meta[ends[number]] = entry
                    ends[number] += jnp.where(target < slots, 1, 0)
        for number in range(len(products)):
            for u in range(GROUP):
                meta[ends[number] + u] = slots
            meta[lay.counts[number] + s] = ends[number] - starts[number]
        if lay.kept is not None:
            for which in range(n):
                for k in range(slots):
                    slot_of[cols[which][here + s, k]] = k
                for j in range(per):
                    at = lay.kept + (which * slab + s) * per + j
                    meta[at] = slot_of[outs[which][s, rep * per + j]]
                for k in range(slots):
                    slot_of[cols[which][here + s, k]] = slots
        for which in range(n):
            for j in range(slots):
                inverse[which][outs[which][s, j]] = slots
        return carry

    lax.fori_loop(0, slab, row, 0)


def planned(lay, reach, window_rows, products, table, row_slot, cols, outs):
    rows, slots = cols[0].shape
    n = len(cols)
    smem, any_spec = pl.BlockSpec(memory_space=pltpu.SMEM), pl.BlockSpec(memory_space=pl.ANY)
    width = 2 * reach + 1
    return pl.pallas_call(
        functools.partial(plan_kernel, lay, reach, window_rows, products),
        in_specs=[smem, smem] + [any_spec] * n + [smem] * n,
        out_specs=smem,
        out_shape=jax.ShapeDtypeStruct((lay.size,), jnp.int32),
        scratch_shapes=[pltpu.SMEM((width * lay.slab, slots), jnp.int32)] * n
        + [pltpu.SMEM((rows,), jnp.int32)] * (n + 1)
        + [pltpu.SemaphoreType.DMA((n * width,))],
        compiler_params=pltpu.CompilerParams(vmem_limit_bytes=VMEM_LIMIT),
        cost_estimate=pl.CostEstimate(flops=4_000_000_000, bytes_accessed=65536, transcendentals=0),
        name="plan",
    )(jnp.asarray(table), row_slot, *cols, *outs)


def kept_kernel(lay, meta, p_ref, d_ref, out_ref, held, sems, out_sem):
    slab, slots, per = lay.slab, lay.slots, lay.per
    loads = []
    for which, blocks in enumerate((p_ref, d_ref)):
        for s in range(slab):
            for j in range(per):
                n = (which * slab + s) * per + j
                k = meta[lay.kept + n]
                load = pltpu.make_async_copy(
                    blocks.at[s, jnp.minimum(k, slots - 1)], held.at[which, s, j], sems.at[n]
                )
                load.start()
                loads.append((load, k, which, s, j))
    for load, k, which, s, j in loads:
        load.wait()

        @pl.when(k == slots)
        def _():
            held[which, s, j] = jnp.zeros(held.shape[3:], held.dtype)

    store = pltpu.make_async_copy(held, out_ref, out_sem)
    store.start()
    store.wait()


def kept_blocks(lay, meta, p_blocks, d_blocks):
    slab, _, side, _ = p_blocks.shape
    shape = (2, slab, lay.per, side, side)
    return pl.pallas_call(
        functools.partial(kept_kernel, lay),
        in_specs=[pl.BlockSpec(memory_space=pltpu.SMEM)] + [pl.BlockSpec(memory_space=pl.ANY)] * 2,
        out_specs=pl.BlockSpec(memory_space=pl.ANY),
        out_shape=jax.ShapeDtypeStruct(shape, p_blocks.dtype),
        scratch_shapes=[
            pltpu.VMEM(shape, p_blocks.dtype),
            pltpu.SemaphoreType.DMA((2 * slab * lay.per,)),
            pltpu.SemaphoreType.DMA,
        ],
        compiler_params=pltpu.CompilerParams(vmem_limit_bytes=VMEM_LIMIT),
        cost_estimate=pl.CostEstimate(flops=3_000_000_000, bytes_accessed=1 << 21, transcendentals=0),
        name="kept",
    )(meta, p_blocks, d_blocks)


def product_kernel(lay, n_left, sizes, first, halves, meta, *refs):
    left_refs = refs[:n_left]
    pieces = refs[n_left : n_left + n_left * len(sizes)]
    out_refs, (window, total, sems) = refs[-3 - 2 * len(halves) : -3], refs[-3:]
    step = pl.program_id(0)
    row = first + step
    per = lay.per

    @pl.when(step == 0)
    def _():
        copies, base = [], 0
        for index, piece in enumerate(pieces):
            size = sizes[index % len(sizes)]
            copies.append(
                pltpu.make_async_copy(
                    piece, window.at[pl.ds(base * per, size * per)], sems.at[index]
                )
            )
            base += size
        for copy in copies:
            copy.start()
        for copy in copies:
            copy.wait()

    total[...] = jnp.zeros_like(total)
    for n in range(n_left):

        def add_group(group, carry):
            for u in range(GROUP):
                code = meta[lay.lists[n] + row * lay.pitch + group * GROUP + u]
                total[code & 15] += jnp.dot(
                    left_refs[n][0, code >> 13], window[(code >> 4) & 511],
                    preferred_element_type=jnp.float32,
                )
            return carry

        groups = (meta[lay.counts[n] + row] + GROUP - 1) // GROUP
        lax.fori_loop(0, groups, add_group, 0)

    def store(send_ref, keep_ref, order):
        for at, q in enumerate(order):
            ref = keep_ref if at < 2 else send_ref
            for j in range(per):
                ref[at % 2, 0, j] = total[q * per + j].astype(ref.dtype)

    half_rows = lay.slab // 2
    for index, half in enumerate(halves):
        refs_of = out_refs[2 * index], out_refs[2 * index + 1]
        if len(halves) == 1:
            store(*refs_of, HALF_ORDER[half])
        else:
            pl.when(row // half_rows == half)(
                functools.partial(store, *refs_of, HALF_ORDER[half])
            )


HALF_ORDER = ((0, 3, 1, 2), (0, 1, 3, 2))


def block_products(lay, lefts, windows, sizes, meta, halves):
    slab, slots, side, _ = lefts[0].shape
    per = lay.per
    pieces = [piece.reshape(-1, side, side) for window in windows for piece in window]
    rows_in = len(windows) * sum(sizes)
    dtype = lefts[0].dtype
    half_rows = slab // 2
    first, steps = halves[0] * half_rows, len(halves) * half_rows
    any_spec = pl.BlockSpec(memory_space=pl.ANY)
    out_specs = []
    for index in range(len(halves)):
        spec = pl.BlockSpec(
            (2, 1, per, side, side),
            lambda s, *_, low=index * half_rows: (
                0, jnp.clip(s - low, 0, half_rows - 1), 0, 0, 0,
            ),
        )
        out_specs += [spec, spec]
    return pl.pallas_call(
        functools.partial(product_kernel, lay, len(lefts), sizes, first, halves),
        grid_spec=pltpu.PrefetchScalarGridSpec(
            num_scalar_prefetch=1,
            grid=(steps,),
            in_specs=[
                pl.BlockSpec((1, slots, side, side), lambda s, *_: (first + s, 0, 0, 0))
            ] * len(lefts)
            + [any_spec] * len(pieces),
            out_specs=out_specs,
            scratch_shapes=[
                pltpu.VMEM((rows_in * per, side, side), dtype),
                pltpu.VMEM((slots + 1, side, side), jnp.float32),
                pltpu.SemaphoreType.DMA((len(pieces),)),
            ],
        ),
        out_shape=[jax.ShapeDtypeStruct((2, half_rows, per, side, side), jnp.bfloat16)]
        * (2 * len(halves)),
        compiler_params=pltpu.CompilerParams(
            dimension_semantics=("arbitrary",), vmem_limit_bytes=VMEM_LIMIT
        ),
        cost_estimate=pl.CostEstimate(
            flops=8_000_000_000,
            bytes_accessed=2 * (rows_in * per + 2 * slab * slots) * side * side,
            transcendentals=0,
        ),
    )(meta, *lefts, *pieces)


def met(value, flip):
    return lax.ppermute(value, "rep", [(i, i ^ flip) for i in range(lax.axis_size("rep"))])


def finish_kernel(rows, branch_ref, *refs):
    kept_ref, out_ref = refs[-2:]
    step = pl.program_id(0)
    half_steps = pl.num_programs(0) // 2

    def store(keep_ref, first_ref, second_ref):
        for s in range(rows):
            squaring = branch_ref[step * rows + s] == 1
            total = keep_ref[0, s].astype(jnp.float32) + first_ref[0, s].astype(jnp.float32)
            total = total + second_ref[s].astype(jnp.float32)
            kept = kept_ref[0, s].astype(jnp.float32)
            out_ref[s] = jnp.where(squaring, total, 2.0 * kept - total).astype(out_ref.dtype)

    for half in range(2):
        pl.when(step // half_steps == half)(
            functools.partial(store, *refs[3 * half : 3 * half + 3])
        )


def finish(halves, kept, which, branch):
    _, half_rows, per, side, _ = halves[0][0].shape
    slab = 2 * half_rows
    rows = 2
    half_steps = half_rows // rows
    in_specs = []
    for half in range(2):

        def at(s, *_, low=half * half_steps):
            return jnp.clip(s - low, 0, half_steps - 1)

        pair = pl.BlockSpec(
            (1, rows, per, side, side), lambda s, *_, at=at: (0, at(s), 0, 0, 0)
        )
        single = pl.BlockSpec((rows, per, side, side), lambda s, *_, at=at: (at(s), 0, 0, 0))
        in_specs += [pair, pair, single]
    in_specs.append(
        pl.BlockSpec((1, rows, per, side, side), lambda s, *_: (which, s, 0, 0, 0))
    )
    return pl.pallas_call(
        functools.partial(finish_kernel, rows),
        grid_spec=pltpu.PrefetchScalarGridSpec(
            num_scalar_prefetch=1,
            grid=(slab // rows,),
            in_specs=in_specs,
            out_specs=pl.BlockSpec((rows, per, side, side), lambda s, *_: (s, 0, 0, 0)),
        ),
        out_shape=jax.ShapeDtypeStruct((slab, per, side, side), jnp.bfloat16),
        compiler_params=pltpu.CompilerParams(
            dimension_semantics=("arbitrary",), vmem_limit_bytes=VMEM_LIMIT
        ),
        cost_estimate=pl.CostEstimate(flops=2_000_000_000, bytes_accessed=4 << 20, transcendentals=0),
        name="finish",
    )(branch, *halves[0], *halves[1], kept)


def pair_sum(keep, got):
    return (keep[1].astype(jnp.float32) + got[1].astype(jnp.float32)).astype(jnp.bfloat16)


def step(p_blocks, d_blocks, p_cols, d_cols, out_pcols, out_dcols, row_slot, branch):
    slab, slots, _, _ = p_blocks.shape
    per = slots // lax.axis_size("rep")
    margin = slots + 2 * SPREAD_ROWS
    reach = -(-margin // slab)
    far = margin - 2 * slab
    sizes, table = window_table(slab, margin)
    table = table * per
    window_rows = sum(sizes)

    def outer(pieces):
        part, near, rest, edge = pieces
        out1 = swapped(part, -1, 1)
        far2 = swapped(rest, 2, -2)
        near2 = swapped(near, 2, -2)
        out3 = swapped(edge, -3, 3)
        in1 = swapped(part, 1, -1)
        return part, in1, out1, near2, far2, out3

    def inner(pieces):
        return pieces + (swapped(pieces[2], 1, -1), swapped(pieces[4], 1, -1))

    p_pieces, d_pieces = packed(p_blocks, d_blocks, per, far)
    p_window = outer(p_pieces)
    d_window = outer(d_pieces)
    square_lay = Lists(slab, slots, per, 1, False)
    tangent_lay = Lists(slab, slots, per, 2, True)
    square_meta = planned(
        square_lay, reach, window_rows, ((0, 0, 0),), table, row_slot, (p_cols,), (out_pcols,)
    )
    p_window = inner(p_window)
    d_window = inner(d_window)
    square = block_products(square_lay, (p_blocks,), (p_window,), sizes, square_meta, (0, 1))
    square, later_slot = lax.optimization_barrier((square, row_slot))
    sent_a, keep_a, sent_b, keep_b = square
    first_a = met(sent_a, 1)
    first_b = met(sent_b, 3)

    tangent_meta = planned(
        tangent_lay, reach, window_rows, ((0, 1, 1), (1, 0, 1)), table, later_slot,
        (p_cols, d_cols), (out_pcols, out_dcols),
    )
    kept = kept_blocks(tangent_lay, tangent_meta, p_blocks, d_blocks)
    kept, meta_a = lax.optimization_barrier((kept, tangent_meta))
    lefts, windows = (p_blocks, d_blocks), (p_window, d_window)
    tsent_a, tkeep_a = block_products(tangent_lay, lefts, windows, sizes, meta_a, (0,))
    (tsent_a, tkeep_a), (first_a, first_b) = lax.optimization_barrier(
        ((tsent_a, tkeep_a), (first_a, first_b))
    )
    middle_a, middle_b = pair_sum(keep_a, first_a), pair_sum(keep_b, first_b)
    middle_a, middle_b, meta_b = lax.optimization_barrier((middle_a, middle_b, meta_a))
    second_a = met(middle_a, 3)
    second_b = met(middle_b, 1)
    tfirst_a = met(tsent_a, 1)
    tsent_b, tkeep_b = block_products(tangent_lay, lefts, windows, sizes, meta_b, (1,))
    tfirst_b = met(tsent_b, 3)
    tmiddle_a = pair_sum(tkeep_a, tfirst_a)
    tmiddle_b = pair_sum(tkeep_b, tfirst_b)
    tsecond_a = met(tmiddle_a, 3)
    tsecond_b = met(tmiddle_b, 1)
    next_p = finish(
        ((keep_a, first_a, second_a), (keep_b, first_b, second_b)), kept, 0, branch
    )
    next_d = finish(
        ((tkeep_a, tfirst_a, tsecond_a), (tkeep_b, tfirst_b, tsecond_b)), kept, 1, branch
    )
    return next_p, next_d


def solution(mesh):
    return jax.shard_map(
        step,
        mesh=mesh,
        in_specs=(
            P("rows", None, None, None),
            P("rows", None, None, None),
            P(),
            P(),
            P("rows", None),
            P("rows", None),
            P(),
            P("rows"),
        ),
        out_specs=(P("rows", "rep", None, None), P("rows", "rep", None, None)),
        check_vma=False,
    )
```

```python
import functools

import jax
import jax.numpy as jnp
import numpy as np
from jax import lax
from jax.experimental import pallas as pl
from jax.experimental.pallas import tpu as pltpu
from jax.sharding import PartitionSpec as P


SPREAD_ROWS = 3
GROUP = 8
BATCH = 2
VMEM_LIMIT = 67_000_000


def window_table(slab, margin):
    far = margin - 2 * slab
    sizes = (slab, slab, slab, slab - far, far, far, slab, far)
    own, in1, out1, near2, far2, out3, in2, in3 = np.cumsum((0,) + sizes[:-1])

    def run(start, count):
        return list(range(start, start + count))

    core0 = (
        run(out3, far) + run(near2, slab - far) + run(far2, far) + run(out1, slab)
        + run(own, slab) + run(in1, slab) + run(in2, slab) + run(in3, far)
    )
    core1 = (
        run(in3, far) + run(in2, slab) + run(in1, slab) + run(own, slab)
        + run(out1, slab) + run(far2, far) + run(near2, slab - far) + run(out3, far)
    )
    edge = [0] * (slab - far)
    return sizes, np.array(edge + core0 + edge + edge + core1 + edge, np.int32)


def swapped(value, even_step, odd_step):
    count = lax.axis_size("rows")
    pairs = [(i, (i + (odd_step if i % 2 else even_step)) % count) for i in range(count)]
    return lax.ppermute(value, "rows", pairs)


def pack_kernel(far, *refs):
    blocks, outs, (held, sems) = refs[:2], refs[2:10], refs[10:]
    slab, per = held.shape[1:3]
    core, rep = lax.axis_index("rows") % 2, lax.axis_index("rep")
    rest = slab - far
    loads = [
        pltpu.make_async_copy(block.at[:, pl.ds(rep * per, per)], held.at[n], sems.at[n, 4])
        for n, block in enumerate(blocks)
    ]
    for load in loads:
        load.start()
    stores = []
    for n, load in enumerate(loads):
        load.wait()
        cuts = (
            held.at[n],
            held.at[n, pl.ds(core * far, rest)],
            held.at[n, pl.ds((1 - core) * rest, far)],
            held.at[n, pl.ds(core * rest, far)],
        )
        for i, cut in enumerate(cuts):
            store = pltpu.make_async_copy(cut, outs[4 * n + i], sems.at[n, i])
            store.start()
            stores.append(store)
    for store in stores:
        store.wait()


def packed(p_blocks, d_blocks, per, far):
    slab, _, side, _ = p_blocks.shape
    dtype = p_blocks.dtype
    shapes = [(slab, per), (slab - far, per), (far, per), (far, per)] * 2
    outs = pl.pallas_call(
        functools.partial(pack_kernel, far),
        in_specs=[pl.BlockSpec(memory_space=pl.ANY)] * 2,
        out_specs=[pl.BlockSpec(memory_space=pl.ANY)] * 8,
        out_shape=[jax.ShapeDtypeStruct(s + (side, side), dtype) for s in shapes],
        scratch_shapes=[
            pltpu.VMEM((2, slab, per, side, side), dtype),
            pltpu.SemaphoreType.DMA((2, 5)),
        ],
        compiler_params=pltpu.CompilerParams(vmem_limit_bytes=VMEM_LIMIT),
        cost_estimate=pl.CostEstimate(flops=3_000_000_000, bytes_accessed=1 << 22, transcendentals=0),
        name="pack",
    )(p_blocks, d_blocks)
    return outs[:4], outs[4:]


class Lists:
    def __init__(self, slab, slots, per, n_products, kept):
        self.slab, self.slots, self.per = slab, slots, per
        self.pitch = n_products * slots * per + GROUP
        self.kept = slab if kept else None
        self.list = slab + (2 * slab * per if kept else 0)
        self.size = self.list + slab * self.pitch


def plan_kernel(lay, reach, window_rows, products, table, row_slot, *refs):
    n = 1 + max(max(product) for product in products)
    cols_hbm, outs = refs[:n], refs[n : 2 * n]
    meta = refs[2 * n]
    cols, inverse, (slot_of, sems) = refs[2 * n + 1 : 3 * n + 1], refs[3 * n + 1 : 4 * n + 1], refs[-2:]
    slab, slots, per = lay.slab, lay.slots, lay.per
    rows = row_slot.shape[0]
    index, rep = lax.axis_index("rows"), lax.axis_index("rep")
    row_start = index * slab
    slabs = rows // slab
    width = 2 * reach + 1
    table_base = (index % 2) * (width * slab)

    copies = []
    for which in range(n):
        for near in range(width):
            at = (index + near + slabs - reach) & (slabs - 1)
            copies.append(
                pltpu.make_async_copy(
                    cols_hbm[which].at[pl.ds(at * slab, slab)],
                    cols[which].at[pl.ds(near * slab, slab)],
                    sems.at[which * width + near],
                )
            )
    for copy in copies:
        copy.start()
    span = 2 * slots + SPREAD_ROWS
    for column in range(-span, slab + span):
        for inv in inverse + ((slot_of,) if lay.kept is not None else ()):
            inv[(row_start + column + rows) & (rows - 1)] = slots
    for copy in copies:
        copy.wait()
    relative = [(q ^ rep) * per for q in range(slots // per)]
    here = reach * slab

    def row(s, carry):
        for which in range(n):
            for j in range(slots):
                inverse[which][outs[which][s, j]] = relative[j // per] + j % per
        start = lay.list + s * lay.pitch
        end = start
        lefts = sorted({product[0] for product in products})
        for first in range(0, slots, BATCH):
            found = []
            for k in range(first, min(first + BATCH, slots)):
                for left in lefts:
                    column = cols[left][here + s, k]
                    offset = (row_slot[column] - row_start + here + rows) & (rows - 1)
                    code = (table[table_base + offset] << 4) + ((left * slots + k) << 13)
                    for which_left, right, out in products:
                        if which_left != left:
                            continue
                        base = right * window_rows * per if n > 1 else 0
                        for m in range(per):
                            target = inverse[out][cols[right][offset, rep * per + m]]
                            found.append((target, code + ((base + m) << 4)))
            for target, entry in found:
                meta[end] = entry + target
                end += jnp.where(target < slots, 1, 0)
        for u in range(GROUP):
            meta[end + u] = slots
        meta[s] = end - start
        if lay.kept is not None:
            for which in range(n):
                for k in range(slots):
                    slot_of[cols[which][here + s, k]] = k
                for j in range(per):
                    at = lay.kept + (which * slab + s) * per + j
                    meta[at] = slot_of[outs[which][s, rep * per + j]]
                for k in range(slots):
                    slot_of[cols[which][here + s, k]] = slots
        for which in range(n):
            for j in range(slots):
                inverse[which][outs[which][s, j]] = slots
        return carry

    lax.fori_loop(0, slab, row, 0)


def planned(lay, reach, window_rows, products, table, row_slot, cols, outs):
    rows, slots = cols[0].shape
    n = len(cols)
    smem, any_spec = pl.BlockSpec(memory_space=pltpu.SMEM), pl.BlockSpec(memory_space=pl.ANY)
    width = 2 * reach + 1
    return pl.pallas_call(
        functools.partial(plan_kernel, lay, reach, window_rows, products),
        in_specs=[smem, smem] + [any_spec] * n + [smem] * n,
        out_specs=smem,
        out_shape=jax.ShapeDtypeStruct((lay.size,), jnp.int32),
        scratch_shapes=[pltpu.SMEM((width * lay.slab, slots), jnp.int32)] * n
        + [pltpu.SMEM((rows,), jnp.int32)] * (n + 1)
        + [pltpu.SemaphoreType.DMA((n * width,))],
        compiler_params=pltpu.CompilerParams(vmem_limit_bytes=VMEM_LIMIT),
        cost_estimate=pl.CostEstimate(flops=4_000_000_000, bytes_accessed=65536, transcendentals=0),
        name="plan",
    )(jnp.asarray(table), row_slot, *cols, *outs)


def kept_kernel(lay, meta, p_ref, d_ref, out_ref, held, sems, out_sem):
    slab, slots, per = lay.slab, lay.slots, lay.per
    loads = []
    for which, blocks in enumerate((p_ref, d_ref)):
        for s in range(slab):
            for j in range(per):
                n = (which * slab + s) * per + j
                k = meta[lay.kept + n]
                load = pltpu.make_async_copy(
                    blocks.at[s, jnp.minimum(k, slots - 1)], held.at[which, s, j], sems.at[n]
                )
                load.start()
                loads.append((load, k, which, s, j))
    for load, k, which, s, j in loads:
        load.wait()

        @pl.when(k == slots)
        def _():
            held[which, s, j] = jnp.zeros(held.shape[3:], held.dtype)

    store = pltpu.make_async_copy(held, out_ref, out_sem)
    store.start()
    store.wait()


def kept_blocks(lay, meta, p_blocks, d_blocks):
    slab, _, side, _ = p_blocks.shape
    shape = (2, slab, lay.per, side, side)
    return pl.pallas_call(
        functools.partial(kept_kernel, lay),
        in_specs=[pl.BlockSpec(memory_space=pltpu.SMEM)] + [pl.BlockSpec(memory_space=pl.ANY)] * 2,
        out_specs=pl.BlockSpec(memory_space=pl.ANY),
        out_shape=jax.ShapeDtypeStruct(shape, p_blocks.dtype),
        scratch_shapes=[
            pltpu.VMEM(shape, p_blocks.dtype),
            pltpu.SemaphoreType.DMA((2 * slab * lay.per,)),
            pltpu.SemaphoreType.DMA,
        ],
        compiler_params=pltpu.CompilerParams(vmem_limit_bytes=VMEM_LIMIT),
        cost_estimate=pl.CostEstimate(flops=3_000_000_000, bytes_accessed=1 << 21, transcendentals=0),
        name="kept",
    )(meta, p_blocks, d_blocks)


def product_kernel(lay, n_left, sizes, meta, *refs):
    left_refs = refs[:n_left]
    pieces = refs[n_left : n_left + n_left * len(sizes)]
    outs, stages = refs[-12:-8], refs[-8:-4]
    left, window, total, sems = refs[-4:]
    slab, slots, per = lay.slab, lay.slots, lay.per
    half_rows = slab // 2
    window_sem, left_sem, out_sem = 0, len(pieces), len(pieces) + slab * n_left

    def left_copy(row, n):
        return pltpu.make_async_copy(
            left_refs[n].at[row], left.at[row, pl.ds(n * slots, slots)],
            sems.at[left_sem + row * n_left + n],
        )

    copies, base = [], 0
    for index, piece in enumerate(pieces):
        size = sizes[index % len(sizes)]
        copies.append(
            pltpu.make_async_copy(
                piece, window.at[pl.ds(base * per, size * per)], sems.at[window_sem + index]
            )
        )
        base += size
    for copy in copies:
        copy.start()
    for row in range(slab):
        for n in range(n_left):
            left_copy(row, n).start()
    for copy in copies:
        copy.wait()

    def out_copy(half, row, which):
        number = 2 * half + which
        return pltpu.make_async_copy(
            stages[number].at[:, row], outs[number].at[:, row],
            sems.at[out_sem + (half * half_rows + row) * 2 + which],
        )

    for half in range(2):

        def one_row(local_row, carry):
            row = half * half_rows + local_row
            for n in range(n_left):
                left_copy(row, n).wait()
            total[...] = jnp.zeros_like(total)

            def add_group(group, inner):
                for u in range(GROUP):
                    code = meta[lay.list + row * lay.pitch + group * GROUP + u]
                    total[code & 15] += jnp.dot(
                        left[row, code >> 13], window[(code >> 4) & 511],
                        preferred_element_type=jnp.float32,
                    )
                return inner

            lax.fori_loop(0, (meta[row] + GROUP - 1) // GROUP, add_group, 0)
            for at, q in enumerate(HALF_ORDER[half]):
                stage = stages[2 * half + (1 if at < 2 else 0)]
                for j in range(per):
                    stage[at % 2, local_row, j] = total[q * per + j].astype(stage.dtype)
            for which in range(2):
                out_copy(half, local_row, which).start()
            return carry

        lax.fori_loop(0, half_rows, one_row, 0)
    for half in range(2):
        for row in range(half_rows):
            for which in range(2):
                out_copy(half, row, which).wait()


HALF_ORDER = ((0, 3, 1, 2), (0, 1, 3, 2))


def block_products(lay, lefts, windows, sizes, meta):
    slab, slots, side, _ = lefts[0].shape
    per = lay.per
    pieces = [piece.reshape(-1, side, side) for window in windows for piece in window]
    rows_in = len(windows) * sum(sizes)
    dtype = lefts[0].dtype
    any_spec = pl.BlockSpec(memory_space=pl.ANY)
    out_shape = (2, slab // 2, per, side, side)
    return pl.pallas_call(
        functools.partial(product_kernel, lay, len(lefts), sizes),
        in_specs=[pl.BlockSpec(memory_space=pltpu.SMEM)]
        + [any_spec] * (len(lefts) + len(pieces)),
        out_specs=[any_spec] * 4,
        scratch_shapes=[pltpu.VMEM(out_shape, jnp.bfloat16)] * 4
        + [
            pltpu.VMEM((slab, len(lefts) * slots, side, side), dtype),
            pltpu.VMEM((rows_in * per, side, side), dtype),
            pltpu.VMEM((slots + 1, side, side), jnp.float32),
            pltpu.SemaphoreType.DMA((len(pieces) + slab * len(lefts) + 2 * slab,)),
        ],
        out_shape=[jax.ShapeDtypeStruct(out_shape, jnp.bfloat16)] * 4,
        compiler_params=pltpu.CompilerParams(vmem_limit_bytes=VMEM_LIMIT),
        cost_estimate=pl.CostEstimate(
            flops=8_000_000_000,
            bytes_accessed=2 * (rows_in * per + 2 * slab * slots) * side * side,
            transcendentals=0,
        ),
    )(meta, *lefts, *pieces)


def met(value, flip):
    return lax.ppermute(value, "rep", [(i, i ^ flip) for i in range(lax.axis_size("rep"))])


def finish_kernel(which, branch_ref, *refs):
    sources, (kept_ref, out_ref) = refs[:6], refs[6:8]
    parts, kept, out, sems = refs[8:]
    half_rows = out.shape[1]
    loads = []
    for half in range(2):
        for i in range(3):
            source = sources[3 * half + i]
            loads.append(
                pltpu.make_async_copy(
                    source if i == 2 else source.at[0], parts.at[half, i], sems.at[half, i]
                )
            )
        rows = pl.ds(half * half_rows, half_rows)
        loads.append(
            pltpu.make_async_copy(kept_ref.at[which, rows], kept.at[half], sems.at[half, 3])
        )
    for load in loads:
        load.start()
    stores = []
    for half in range(2):
        for load in loads[4 * half : 4 * half + 4]:
            load.wait()
        for row in range(half_rows):
            squaring = branch_ref[half * half_rows + row] == 1
            total = parts[half, 0, row].astype(jnp.float32) + parts[half, 1, row].astype(jnp.float32)
            total = total + parts[half, 2, row].astype(jnp.float32)
            twice = 2.0 * kept[half, row].astype(jnp.float32)
            out[half, row] = jnp.where(squaring, total, twice - total).astype(out.dtype)
            store = pltpu.make_async_copy(
                out.at[half, row], out_ref.at[half * half_rows + row],
                sems.at[half, 4 + row],
            )
            store.start()
            stores.append(store)
    for store in stores:
        store.wait()


def finish(halves, kept, which, branch):
    _, half_rows, per, side, _ = halves[0][0].shape
    dtype = jnp.bfloat16
    any_spec = pl.BlockSpec(memory_space=pl.ANY)
    half = (half_rows, per, side, side)
    return pl.pallas_call(
        functools.partial(finish_kernel, which),
        in_specs=[pl.BlockSpec(memory_space=pltpu.SMEM)] + [any_spec] * 7,
        out_specs=any_spec,
        out_shape=jax.ShapeDtypeStruct((2 * half_rows, per, side, side), dtype),
        scratch_shapes=[
            pltpu.VMEM((2, 3) + half, dtype),
            pltpu.VMEM((2,) + half, dtype),
            pltpu.VMEM((2,) + half, dtype),
            pltpu.SemaphoreType.DMA((2, 4 + half_rows)),
        ],
        compiler_params=pltpu.CompilerParams(vmem_limit_bytes=VMEM_LIMIT),
        cost_estimate=pl.CostEstimate(flops=2_000_000_000, bytes_accessed=4 << 20, transcendentals=0),
        name="finish",
    )(branch, *halves[0], *halves[1], kept)


def pair_sum(keep, got):
    return (keep[1].astype(jnp.float32) + got[1].astype(jnp.float32)).astype(jnp.bfloat16)


def step(p_blocks, d_blocks, p_cols, d_cols, out_pcols, out_dcols, row_slot, branch):
    slab, slots, _, _ = p_blocks.shape
    per = slots // lax.axis_size("rep")
    margin = slots + 2 * SPREAD_ROWS
    reach = -(-margin // slab)
    far = margin - 2 * slab
    sizes, table = window_table(slab, margin)
    table = table * per
    window_rows = sum(sizes)

    def outer(pieces):
        part, near, rest, edge = pieces
        out1 = swapped(part, -1, 1)
        far2 = swapped(rest, 2, -2)
        near2 = swapped(near, 2, -2)
        out3 = swapped(edge, -3, 3)
        in1 = swapped(part, 1, -1)
        return part, in1, out1, near2, far2, out3

    def inner(pieces):
        return pieces + (swapped(pieces[2], 1, -1), swapped(pieces[4], 1, -1))

    p_pieces, d_pieces = packed(p_blocks, d_blocks, per, far)
    p_window = outer(p_pieces)
    d_window = outer(d_pieces)
    square_lay = Lists(slab, slots, per, 1, False)
    tangent_lay = Lists(slab, slots, per, 2, True)
    square_meta = planned(
        square_lay, reach, window_rows, ((0, 0, 0),), table, row_slot, (p_cols,), (out_pcols,)
    )
    tangent_meta = planned(
        tangent_lay, reach, window_rows, ((0, 1, 1), (1, 0, 1)), table, row_slot,
        (p_cols, d_cols), (out_pcols, out_dcols),
    )
    p_window = inner(p_window)
    d_window = inner(d_window)
    sent_a, keep_a, sent_b, keep_b = block_products(
        square_lay, (p_blocks,), (p_window,), sizes, square_meta
    )
    first_a = met(sent_a, 1)
    first_b = met(sent_b, 3)
    keep_a, kept_meta = lax.optimization_barrier((keep_a, tangent_meta))
    kept = kept_blocks(tangent_lay, kept_meta, p_blocks, d_blocks)
    kept, tangent_meta = lax.optimization_barrier((kept, tangent_meta))
    tsent_a, tkeep_a, tsent_b, tkeep_b = block_products(
        tangent_lay, (p_blocks, d_blocks), (p_window, d_window), sizes, tangent_meta,
    )
    tfirst_a = met(tsent_a, 1)
    tfirst_b = met(tsent_b, 3)
    second_a = met(pair_sum(keep_a, first_a), 3)
    second_b = met(pair_sum(keep_b, first_b), 1)
    tsecond_a = met(pair_sum(tkeep_a, tfirst_a), 3)
    tsecond_b = met(pair_sum(tkeep_b, tfirst_b), 1)
    next_p = finish(
        ((keep_a, first_a, second_a), (keep_b, first_b, second_b)), kept, 0, branch
    )
    next_d = finish(
        ((tkeep_a, tfirst_a, tsecond_a), (tkeep_b, tfirst_b, tsecond_b)), kept, 1, branch
    )
    return next_p, next_d


def solution(mesh):
    return jax.shard_map(
        step,
        mesh=mesh,
        in_specs=(
            P("rows", None, None, None),
            P("rows", None, None, None),
            P(),
            P(),
            P("rows", None),
            P("rows", None),
            P(),
            P("rows"),
        ),
        out_specs=(P("rows", "rep", None, None), P("rows", "rep", None, None)),
        check_vma=False,
    )
```

```python
import functools

import jax
import jax.numpy as jnp
import numpy as np
from jax import lax
from jax.experimental import pallas as pl
from jax.experimental.pallas import tpu as pltpu
from jax.sharding import PartitionSpec as P


SPREAD_ROWS = 3
GROUP = 8
BATCH = 2
VMEM_LIMIT = 67_000_000


def window_table(slab, margin):
    far = margin - 2 * slab
    sizes = (slab, slab, slab, slab - far, far, far, slab, far)
    own, in1, out1, near2, far2, out3, in2, in3 = np.cumsum((0,) + sizes[:-1])

    def run(start, count):
        return list(range(start, start + count))

    core0 = (
        run(out3, far) + run(near2, slab - far) + run(far2, far) + run(out1, slab)
        + run(own, slab) + run(in1, slab) + run(in2, slab) + run(in3, far)
    )
    core1 = (
        run(in3, far) + run(in2, slab) + run(in1, slab) + run(own, slab)
        + run(out1, slab) + run(far2, far) + run(near2, slab - far) + run(out3, far)
    )
    edge = [0] * (slab - far)
    return sizes, np.array(edge + core0 + edge + edge + core1 + edge, np.int32)


def swapped(value, even_step, odd_step):
    count = lax.axis_size("rows")
    pairs = [(i, (i + (odd_step if i % 2 else even_step)) % count) for i in range(count)]
    return lax.ppermute(value, "rows", pairs)


def pack_kernel(far, *refs):
    blocks, outs, (held, sems) = refs[:2], refs[2:10], refs[10:]
    slab, per = held.shape[1:3]
    core, rep = lax.axis_index("rows") % 2, lax.axis_index("rep")
    rest = slab - far
    loads = [
        pltpu.make_async_copy(block.at[:, pl.ds(rep * per, per)], held.at[n], sems.at[n, 4])
        for n, block in enumerate(blocks)
    ]
    for load in loads:
        load.start()
    stores = []
    for n, load in enumerate(loads):
        load.wait()
        cuts = (
            held.at[n],
            held.at[n, pl.ds(core * far, rest)],
            held.at[n, pl.ds((1 - core) * rest, far)],
            held.at[n, pl.ds(core * rest, far)],
        )
        for i, cut in enumerate(cuts):
            store = pltpu.make_async_copy(cut, outs[4 * n + i], sems.at[n, i])
            store.start()
            stores.append(store)
    for store in stores:
        store.wait()


def packed(p_blocks, d_blocks, per, far):
    slab, _, side, _ = p_blocks.shape
    dtype = p_blocks.dtype
    shapes = [(slab, per), (slab - far, per), (far, per), (far, per)] * 2
    outs = pl.pallas_call(
        functools.partial(pack_kernel, far),
        in_specs=[pl.BlockSpec(memory_space=pl.ANY)] * 2,
        out_specs=[pl.BlockSpec(memory_space=pl.ANY)] * 8,
        out_shape=[jax.ShapeDtypeStruct(s + (side, side), dtype) for s in shapes],
        scratch_shapes=[
            pltpu.VMEM((2, slab, per, side, side), dtype),
            pltpu.SemaphoreType.DMA((2, 5)),
        ],
        compiler_params=pltpu.CompilerParams(vmem_limit_bytes=VMEM_LIMIT),
        cost_estimate=pl.CostEstimate(flops=3_000_000_000, bytes_accessed=1 << 22, transcendentals=0),
        name="pack",
    )(p_blocks, d_blocks)
    return outs[:4], outs[4:]


class Lists:
    def __init__(self, slab, slots, per, n_products, kept):
        self.slab, self.slots, self.per = slab, slots, per
        self.pitch = n_products * slots * per + GROUP
        self.kept = slab if kept else None
        self.list = slab + (2 * slab * per if kept else 0)
        self.size = self.list + slab * self.pitch


def plan_kernel(lay, reach, window_rows, products, n, table, row_slot, *refs):
    cols, outs, meta = refs[:n], refs[n : 2 * n], refs[2 * n]
    inverse, slot_of = refs[2 * n + 1 : 3 * n + 1], refs[-1]
    slab, slots, per = lay.slab, lay.slots, lay.per
    rows = row_slot.shape[0]
    index, rep = lax.axis_index("rows"), lax.axis_index("rep")
    row_start = index * slab
    here = reach * slab
    table_base = (index % 2) * (2 * here + slab)
    span = 2 * slots + SPREAD_ROWS
    for column in range(-span, slab + span):
        for inv in inverse + ((slot_of,) if lay.kept is not None else ()):
            inv[(row_start + column + rows) & (rows - 1)] = slots
    relative = [(q ^ rep) * per for q in range(slots // per)]

    def row(s, carry):
        own = row_start + s
        for which in range(n):
            for j in range(slots):
                inverse[which][outs[which][s, j]] = relative[j // per] + j % per
        start = lay.list + s * lay.pitch
        end = start
        lefts = sorted({product[0] for product in products})
        for first in range(0, slots, BATCH):
            found = []
            for k in range(first, min(first + BATCH, slots)):
                for left in lefts:
                    stored = row_slot[cols[left][k, own]]
                    offset = (stored - row_start + here + rows) & (rows - 1)
                    code = (table[table_base + offset] << 4) + ((left * slots + k) << 13)
                    for which_left, right, out in products:
                        if which_left != left:
                            continue
                        base = right * window_rows * per if n > 1 else 0
                        for m in range(per):
                            target = inverse[out][cols[right][rep * per + m, stored]]
                            found.append((target, code + ((base + m) << 4)))
            for target, entry in found:
                meta[end] = entry + target
                end += jnp.where(target < slots, 1, 0)
        for u in range(GROUP):
            meta[end + u] = slots
        meta[s] = end - start
        if lay.kept is not None:
            for which in range(n):
                for k in range(slots):
                    slot_of[cols[which][k, own]] = k
                for j in range(per):
                    at = lay.kept + (which * slab + s) * per + j
                    meta[at] = slot_of[outs[which][s, rep * per + j]]
                for k in range(slots):
                    slot_of[cols[which][k, own]] = slots
        for which in range(n):
            for j in range(slots):
                inverse[which][outs[which][s, j]] = slots
        return carry

    lax.fori_loop(0, slab, row, 0)


def planned(lay, reach, window_rows, products, table, row_slot, cols, outs):
    n = len(cols)
    rows = row_slot.shape[0]
    smem = pl.BlockSpec(memory_space=pltpu.SMEM)
    return pl.pallas_call(
        functools.partial(plan_kernel, lay, reach, window_rows, products, n),
        in_specs=[smem] * (2 + 2 * n),
        out_specs=smem,
        out_shape=jax.ShapeDtypeStruct((lay.size,), jnp.int32),
        scratch_shapes=[pltpu.SMEM((rows,), jnp.int32)] * (n + 1),
        compiler_params=pltpu.CompilerParams(vmem_limit_bytes=VMEM_LIMIT),
        cost_estimate=pl.CostEstimate(flops=4_000_000_000, bytes_accessed=65536, transcendentals=0),
        name="plan",
    )(jnp.asarray(table), row_slot, *(ids.T for ids in cols), *outs)


def kept_kernel(lay, meta, p_ref, d_ref, out_ref, held, sems, out_sem):
    slab, slots, per = lay.slab, lay.slots, lay.per
    loads = []
    for which, blocks in enumerate((p_ref, d_ref)):
        for s in range(slab):
            for j in range(per):
                n = (which * slab + s) * per + j
                k = meta[lay.kept + n]
                load = pltpu.make_async_copy(
                    blocks.at[s, jnp.minimum(k, slots - 1)], held.at[which, s, j], sems.at[n]
                )
                load.start()
                loads.append((load, k, which, s, j))
    for load, k, which, s, j in loads:
        load.wait()

        @pl.when(k == slots)
        def _():
            held[which, s, j] = jnp.zeros(held.shape[3:], held.dtype)

    store = pltpu.make_async_copy(held, out_ref, out_sem)
    store.start()
    store.wait()


def kept_blocks(lay, meta, p_blocks, d_blocks):
    slab, _, side, _ = p_blocks.shape
    shape = (2, slab, lay.per, side, side)
    return pl.pallas_call(
        functools.partial(kept_kernel, lay),
        in_specs=[pl.BlockSpec(memory_space=pltpu.SMEM)] + [pl.BlockSpec(memory_space=pl.ANY)] * 2,
        out_specs=pl.BlockSpec(memory_space=pl.ANY),
        out_shape=jax.ShapeDtypeStruct(shape, p_blocks.dtype),
        scratch_shapes=[
            pltpu.VMEM(shape, p_blocks.dtype),
            pltpu.SemaphoreType.DMA((2 * slab * lay.per,)),
            pltpu.SemaphoreType.DMA,
        ],
        compiler_params=pltpu.CompilerParams(vmem_limit_bytes=VMEM_LIMIT),
        cost_estimate=pl.CostEstimate(flops=3_000_000_000, bytes_accessed=1 << 21, transcendentals=0),
        name="kept",
    )(meta, p_blocks, d_blocks)


def product_kernel(lay, n_left, sizes, meta, *refs):
    left_refs = refs[:n_left]
    pieces = refs[n_left : n_left + n_left * len(sizes)]
    outs, stages = refs[-12:-8], refs[-8:-4]
    left, window, total, sems = refs[-4:]
    slab, slots, per = lay.slab, lay.slots, lay.per
    half_rows = slab // 2
    window_sem, left_sem, out_sem = 0, len(pieces), len(pieces) + slab * n_left

    def left_copy(row, n):
        return pltpu.make_async_copy(
            left_refs[n].at[row], left.at[row, pl.ds(n * slots, slots)],
            sems.at[left_sem + row * n_left + n],
        )

    copies, base = [], 0
    for index, piece in enumerate(pieces):
        size = sizes[index % len(sizes)]
        copies.append(
            pltpu.make_async_copy(
                piece, window.at[pl.ds(base * per, size * per)], sems.at[window_sem + index]
            )
        )
        base += size
    for copy in copies:
        copy.start()
    for row in range(slab):
        for n in range(n_left):
            left_copy(row, n).start()
    for copy in copies:
        copy.wait()

    def out_copy(half, row, which):
        number = 2 * half + which
        return pltpu.make_async_copy(
            stages[number].at[:, row], outs[number].at[:, row],
            sems.at[out_sem + (half * half_rows + row) * 2 + which],
        )

    for half in range(2):

        def one_row(local_row, carry):
            row = half * half_rows + local_row
            for n in range(n_left):
                left_copy(row, n).wait()
            total[...] = jnp.zeros_like(total)

            def add_group(group, inner):
                for u in range(GROUP):
                    code = meta[lay.list + row * lay.pitch + group * GROUP + u]
                    total[code & 15] += jnp.dot(
                        left[row, code >> 13], window[(code >> 4) & 511],
                        preferred_element_type=jnp.float32,
                    )
                return inner

            lax.fori_loop(0, (meta[row] + GROUP - 1) // GROUP, add_group, 0)
            for at, q in enumerate(HALF_ORDER[half]):
                stage = stages[2 * half + (1 if at < 2 else 0)]
                for j in range(per):
                    stage[at % 2, local_row, j] = total[q * per + j].astype(stage.dtype)
            for which in range(2):
                out_copy(half, local_row, which).start()
            return carry

        lax.fori_loop(0, half_rows, one_row, 0)
    for half in range(2):
        for row in range(half_rows):
            for which in range(2):
                out_copy(half, row, which).wait()


HALF_ORDER = ((0, 3, 1, 2), (0, 1, 3, 2))


def block_products(lay, lefts, windows, sizes, meta):
    slab, slots, side, _ = lefts[0].shape
    per = lay.per
    pieces = [piece.reshape(-1, side, side) for window in windows for piece in window]
    rows_in = len(windows) * sum(sizes)
    dtype = lefts[0].dtype
    any_spec = pl.BlockSpec(memory_space=pl.ANY)
    out_shape = (2, slab // 2, per, side, side)
    return pl.pallas_call(
        functools.partial(product_kernel, lay, len(lefts), sizes),
        in_specs=[pl.BlockSpec(memory_space=pltpu.SMEM)]
        + [any_spec] * (len(lefts) + len(pieces)),
        out_specs=[any_spec] * 4,
        scratch_shapes=[pltpu.VMEM(out_shape, jnp.bfloat16)] * 4
        + [
            pltpu.VMEM((slab, len(lefts) * slots, side, side), dtype),
            pltpu.VMEM((rows_in * per, side, side), dtype),
            pltpu.VMEM((slots + 1, side, side), jnp.float32),
            pltpu.SemaphoreType.DMA((len(pieces) + slab * len(lefts) + 2 * slab,)),
        ],
        out_shape=[jax.ShapeDtypeStruct(out_shape, jnp.bfloat16)] * 4,
        compiler_params=pltpu.CompilerParams(vmem_limit_bytes=VMEM_LIMIT),
        cost_estimate=pl.CostEstimate(
            flops=8_000_000_000,
            bytes_accessed=2 * (rows_in * per + 2 * slab * slots) * side * side,
            transcendentals=0,
        ),
    )(meta, *lefts, *pieces)


def met(value, flip):
    return lax.ppermute(value, "rep", [(i, i ^ flip) for i in range(lax.axis_size("rep"))])


def finish_kernel(which, branch_ref, *refs):
    sources, (kept_ref, out_ref) = refs[:6], refs[6:8]
    parts, kept, out, sems = refs[8:]
    half_rows = out.shape[1]
    loads = []
    for half in range(2):
        for i in range(3):
            source = sources[3 * half + i]
            loads.append(
                pltpu.make_async_copy(
                    source if i == 2 else source.at[0], parts.at[half, i], sems.at[half, i]
                )
            )
        rows = pl.ds(half * half_rows, half_rows)
        loads.append(
            pltpu.make_async_copy(kept_ref.at[which, rows], kept.at[half], sems.at[half, 3])
        )
    for load in loads:
        load.start()
    stores = []
    for half in range(2):
        for load in loads[4 * half : 4 * half + 4]:
            load.wait()
        for row in range(half_rows):
            squaring = branch_ref[half * half_rows + row] == 1
            total = parts[half, 0, row].astype(jnp.float32) + parts[half, 1, row].astype(jnp.float32)
            total = total + parts[half, 2, row].astype(jnp.float32)
            twice = 2.0 * kept[half, row].astype(jnp.float32)
            out[half, row] = jnp.where(squaring, total, twice - total).astype(out.dtype)
            store = pltpu.make_async_copy(
                out.at[half, row], out_ref.at[half * half_rows + row],
                sems.at[half, 4 + row],
            )
            store.start()
            stores.append(store)
    for store in stores:
        store.wait()


def finish(halves, kept, which, branch):
    _, half_rows, per, side, _ = halves[0][0].shape
    dtype = jnp.bfloat16
    any_spec = pl.BlockSpec(memory_space=pl.ANY)
    half = (half_rows, per, side, side)
    return pl.pallas_call(
        functools.partial(finish_kernel, which),
        in_specs=[pl.BlockSpec(memory_space=pltpu.SMEM)] + [any_spec] * 7,
        out_specs=any_spec,
        out_shape=jax.ShapeDtypeStruct((2 * half_rows, per, side, side), dtype),
        scratch_shapes=[
            pltpu.VMEM((2, 3) + half, dtype),
            pltpu.VMEM((2,) + half, dtype),
            pltpu.VMEM((2,) + half, dtype),
            pltpu.SemaphoreType.DMA((2, 4 + half_rows)),
        ],
        compiler_params=pltpu.CompilerParams(vmem_limit_bytes=VMEM_LIMIT),
        cost_estimate=pl.CostEstimate(flops=2_000_000_000, bytes_accessed=4 << 20, transcendentals=0),
        name="finish",
    )(branch, *halves[0], *halves[1], kept)


def pair_sum(keep, got):
    return (keep[1].astype(jnp.float32) + got[1].astype(jnp.float32)).astype(jnp.bfloat16)


def step(p_blocks, d_blocks, p_cols, d_cols, out_pcols, out_dcols, row_slot, branch):
    slab, slots, _, _ = p_blocks.shape
    per = slots // lax.axis_size("rep")
    margin = slots + 2 * SPREAD_ROWS
    reach = -(-margin // slab)
    far = margin - 2 * slab
    sizes, table = window_table(slab, margin)
    table = table * per
    window_rows = sum(sizes)

    def outer(pieces):
        part, near, rest, edge = pieces
        out1 = swapped(part, -1, 1)
        far2 = swapped(rest, 2, -2)
        near2 = swapped(near, 2, -2)
        out3 = swapped(edge, -3, 3)
        in1 = swapped(part, 1, -1)
        return part, in1, out1, near2, far2, out3

    def inner(pieces):
        return pieces + (swapped(pieces[2], 1, -1), swapped(pieces[4], 1, -1))

    p_pieces, d_pieces = packed(p_blocks, d_blocks, per, far)
    p_window = outer(p_pieces)
    d_window = outer(d_pieces)
    square_lay = Lists(slab, slots, per, 1, False)
    tangent_lay = Lists(slab, slots, per, 2, True)
    square_meta = planned(
        square_lay, reach, window_rows, ((0, 0, 0),), table, row_slot, (p_cols,), (out_pcols,)
    )
    p_window = inner(p_window)
    d_window = inner(d_window)
    sent_a, keep_a, sent_b, keep_b = block_products(
        square_lay, (p_blocks,), (p_window,), sizes, square_meta
    )
    first_a = met(sent_a, 1)
    first_b = met(sent_b, 3)
    keep_a, later_slot = lax.optimization_barrier((keep_a, row_slot))
    tangent_meta = planned(
        tangent_lay, reach, window_rows, ((0, 1, 1), (1, 0, 1)), table, later_slot,
        (p_cols, d_cols), (out_pcols, out_dcols),
    )
    tsent_a, tkeep_a, tsent_b, tkeep_b = block_products(
        tangent_lay, (p_blocks, d_blocks), (p_window, d_window), sizes, tangent_meta,
    )
    tkeep_a, kept_meta = lax.optimization_barrier((tkeep_a, tangent_meta))
    kept = kept_blocks(tangent_lay, kept_meta, p_blocks, d_blocks)
    tfirst_a = met(tsent_a, 1)
    tfirst_b = met(tsent_b, 3)
    second_a = met(pair_sum(keep_a, first_a), 3)
    second_b = met(pair_sum(keep_b, first_b), 1)
    tsecond_a = met(pair_sum(tkeep_a, tfirst_a), 3)
    tsecond_b = met(pair_sum(tkeep_b, tfirst_b), 1)
    next_p = finish(
        ((keep_a, first_a, second_a), (keep_b, first_b, second_b)), kept, 0, branch
    )
    next_d = finish(
        ((tkeep_a, tfirst_a, tsecond_a), (tkeep_b, tfirst_b, tsecond_b)), kept, 1, branch
    )
    return next_p, next_d


def solution(mesh):
    return jax.shard_map(
        step,
        mesh=mesh,
        in_specs=(
            P("rows", None, None, None),
            P("rows", None, None, None),
            P(),
            P(),
            P("rows", None),
            P("rows", None),
            P(),
            P("rows"),
        ),
        out_specs=(P("rows", "rep", None, None), P("rows", "rep", None, None)),
        check_vma=False,
    )
```

```python
import functools

import jax
import jax.numpy as jnp
import numpy as np
from jax import lax
from jax.experimental import pallas as pl
from jax.experimental.pallas import tpu as pltpu
from jax.sharding import PartitionSpec as P


SPREAD_ROWS = 3
GROUPS = (16, 32)
BATCH = 2
VMEM_LIMIT = 67_000_000


def window_table(slab, margin):
    far = margin - 2 * slab
    sizes = (slab, slab, slab, slab - far, far, far, slab, far)
    own, in1, out1, near2, far2, out3, in2, in3 = np.cumsum((0,) + sizes[:-1])

    def run(start, count):
        return list(range(start, start + count))

    core0 = (
        run(out3, far) + run(near2, slab - far) + run(far2, far) + run(out1, slab)
        + run(own, slab) + run(in1, slab) + run(in2, slab) + run(in3, far)
    )
    core1 = (
        run(in3, far) + run(in2, slab) + run(in1, slab) + run(own, slab)
        + run(out1, slab) + run(far2, far) + run(near2, slab - far) + run(out3, far)
    )
    edge = [0] * (slab - far)
    return sizes, np.array(edge + core0 + edge + edge + core1 + edge, np.int32)


def swapped(value, even_step, odd_step):
    count = lax.axis_size("rows")
    pairs = [(i, (i + (odd_step if i % 2 else even_step)) % count) for i in range(count)]
    return lax.ppermute(value, "rows", pairs)


def pack_kernel(far, *refs):
    blocks, outs, (held, sems) = refs[:2], refs[2:10], refs[10:]
    slab, per = held.shape[1:3]
    core, rep = lax.axis_index("rows") % 2, lax.axis_index("rep")
    rest = slab - far
    loads = [
        pltpu.make_async_copy(block.at[:, pl.ds(rep * per, per)], held.at[n], sems.at[n, 4])
        for n, block in enumerate(blocks)
    ]
    for load in loads:
        load.start()
    stores = []
    for n, load in enumerate(loads):
        load.wait()
        cuts = (
            held.at[n],
            held.at[n, pl.ds(core * far, rest)],
            held.at[n, pl.ds((1 - core) * rest, far)],
            held.at[n, pl.ds(core * rest, far)],
        )
        for i, cut in enumerate(cuts):
            store = pltpu.make_async_copy(cut, outs[4 * n + i], sems.at[n, i])
            store.start()
            stores.append(store)
    for store in stores:
        store.wait()


def packed(p_blocks, d_blocks, per, far):
    slab, _, side, _ = p_blocks.shape
    dtype = p_blocks.dtype
    shapes = [(slab, per), (slab - far, per), (far, per), (far, per)] * 2
    outs = pl.pallas_call(
        functools.partial(pack_kernel, far),
        in_specs=[pl.BlockSpec(memory_space=pl.ANY)] * 2,
        out_specs=[pl.BlockSpec(memory_space=pl.ANY)] * 8,
        out_shape=[jax.ShapeDtypeStruct(s + (side, side), dtype) for s in shapes],
        scratch_shapes=[
            pltpu.VMEM((2, slab, per, side, side), dtype),
            pltpu.SemaphoreType.DMA((2, 5)),
        ],
        compiler_params=pltpu.CompilerParams(vmem_limit_bytes=VMEM_LIMIT),
        cost_estimate=pl.CostEstimate(flops=3_000_000_000, bytes_accessed=1 << 22, transcendentals=0),
        name="pack",
    )(p_blocks, d_blocks)
    return outs[:4], outs[4:]


class Lists:
    def __init__(self, slab, slots, per, n_products, kept):
        self.slab, self.slots, self.per = slab, slots, per
        self.group = GROUPS[n_products - 1]
        self.pitch = n_products * slots * per + self.group
        self.kept = slab if kept else None
        self.list = slab + (2 * slab * per if kept else 0)
        self.size = self.list + slab * self.pitch


def plan_kernel(lay, reach, window_rows, products, n, table, row_slot, *refs):
    cols, outs, meta = refs[:n], refs[n : 2 * n], refs[2 * n]
    inverse, slot_of = refs[2 * n + 1 : 3 * n + 1], refs[-1]
    slab, slots, per = lay.slab, lay.slots, lay.per
    rows = row_slot.shape[0]
    index, rep = lax.axis_index("rows"), lax.axis_index("rep")
    row_start = index * slab
    here = reach * slab
    table_base = (index % 2) * (2 * here + slab)
    span = 2 * slots + SPREAD_ROWS
    for column in range(-span, slab + span):
        for inv in inverse + ((slot_of,) if lay.kept is not None else ()):
            inv[(row_start + column + rows) & (rows - 1)] = slots
    relative = [(q ^ rep) * per for q in range(slots // per)]

    def row(s, carry):
        own = row_start + s
        for which in range(n):
            for j in range(slots):
                inverse[which][outs[which][s, j]] = relative[j // per] + j % per
        start = lay.list + s * lay.pitch
        end = start
        lefts = sorted({product[0] for product in products})
        for first in range(0, slots, BATCH):
            found = []
            for k in range(first, min(first + BATCH, slots)):
                for left in lefts:
                    stored = row_slot[cols[left][k, own]]
                    offset = (stored - row_start + here + rows) & (rows - 1)
                    code = (table[table_base + offset] << 4) + ((left * slots + k) << 13)
                    for which_left, right, out in products:
                        if which_left != left:
                            continue
                        base = right * window_rows * per if n > 1 else 0
                        for m in range(per):
                            target = inverse[out][cols[right][rep * per + m, stored]]
                            found.append((target, code + ((base + m) << 4)))
            for target, entry in found:
                meta[end] = entry + target
                end += jnp.where(target < slots, 1, 0)
        for u in range(lay.group):
            meta[end + u] = slots
        meta[s] = end - start
        if lay.kept is not None:
            for which in range(n):
                for k in range(slots):
                    slot_of[cols[which][k, own]] = k
                for j in range(per):
                    at = lay.kept + (which * slab + s) * per + j
                    meta[at] = slot_of[outs[which][s, rep * per + j]]
                for k in range(slots):
                    slot_of[cols[which][k, own]] = slots
        for which in range(n):
            for j in range(slots):
                inverse[which][outs[which][s, j]] = slots
        return carry

    lax.fori_loop(0, slab, row, 0)


def planned(lay, reach, window_rows, products, table, row_slot, cols, outs):
    n = len(cols)
    rows = row_slot.shape[0]
    smem = pl.BlockSpec(memory_space=pltpu.SMEM)
    return pl.pallas_call(
        functools.partial(plan_kernel, lay, reach, window_rows, products, n),
        in_specs=[smem] * (2 + 2 * n),
        out_specs=smem,
        out_shape=jax.ShapeDtypeStruct((lay.size,), jnp.int32),
        scratch_shapes=[pltpu.SMEM((rows,), jnp.int32)] * (n + 1),
        compiler_params=pltpu.CompilerParams(vmem_limit_bytes=VMEM_LIMIT),
        cost_estimate=pl.CostEstimate(flops=4_000_000_000, bytes_accessed=65536, transcendentals=0),
        name="plan",
    )(jnp.asarray(table), row_slot, *(ids.T for ids in cols), *outs)


def kept_kernel(lay, meta, p_ref, d_ref, out_ref, held, sems, out_sem):
    slab, slots, per = lay.slab, lay.slots, lay.per
    loads = []
    for which, blocks in enumerate((p_ref, d_ref)):
        for s in range(slab):
            for j in range(per):
                n = (which * slab + s) * per + j
                k = meta[lay.kept + n]
                load = pltpu.make_async_copy(
                    blocks.at[s, jnp.minimum(k, slots - 1)], held.at[which, s, j], sems.at[n]
                )
                load.start()
                loads.append((load, k, which, s, j))
    for load, k, which, s, j in loads:
        load.wait()

        @pl.when(k == slots)
        def _():
            held[which, s, j] = jnp.zeros(held.shape[3:], held.dtype)

    store = pltpu.make_async_copy(held, out_ref, out_sem)
    store.start()
    store.wait()


def kept_blocks(lay, meta, p_blocks, d_blocks):
    slab, _, side, _ = p_blocks.shape
    shape = (2, slab, lay.per, side, side)
    return pl.pallas_call(
        functools.partial(kept_kernel, lay),
        in_specs=[pl.BlockSpec(memory_space=pltpu.SMEM)] + [pl.BlockSpec(memory_space=pl.ANY)] * 2,
        out_specs=pl.BlockSpec(memory_space=pl.ANY),
        out_shape=jax.ShapeDtypeStruct(shape, p_blocks.dtype),
        scratch_shapes=[
            pltpu.VMEM(shape, p_blocks.dtype),
            pltpu.SemaphoreType.DMA((2 * slab * lay.per,)),
            pltpu.SemaphoreType.DMA,
        ],
        compiler_params=pltpu.CompilerParams(vmem_limit_bytes=VMEM_LIMIT),
        cost_estimate=pl.CostEstimate(flops=3_000_000_000, bytes_accessed=1 << 21, transcendentals=0),
        name="kept",
    )(meta, p_blocks, d_blocks)


def product_kernel(lay, n_left, sizes, meta, *refs):
    left_refs = refs[:n_left]
    pieces = refs[n_left : n_left + n_left * len(sizes)]
    outs, stages = refs[-12:-8], refs[-8:-4]
    left, window, total, sems = refs[-4:]
    slab, slots, per = lay.slab, lay.slots, lay.per
    half_rows = slab // 2
    window_sem, left_sem, out_sem = 0, len(pieces), len(pieces) + slab * n_left

    def left_copy(row, n):
        return pltpu.make_async_copy(
            left_refs[n].at[row], left.at[row, pl.ds(n * slots, slots)],
            sems.at[left_sem + row * n_left + n],
        )

    copies, base = [], 0
    for index, piece in enumerate(pieces):
        size = sizes[index % len(sizes)]
        copies.append(
            pltpu.make_async_copy(
                piece, window.at[pl.ds(base * per, size * per)], sems.at[window_sem + index]
            )
        )
        base += size
    for copy in copies:
        copy.start()
    for row in range(slab):
        for n in range(n_left):
            left_copy(row, n).start()
    for copy in copies:
        copy.wait()

    def out_copy(half, row, which):
        number = 2 * half + which
        return pltpu.make_async_copy(
            stages[number].at[:, row], outs[number].at[:, row],
            sems.at[out_sem + (half * half_rows + row) * 2 + which],
        )

    for half in range(2):

        def one_row(local_row, carry):
            row = half * half_rows + local_row
            for n in range(n_left):
                left_copy(row, n).wait()
            total[...] = jnp.zeros_like(total)

            def add_group(group, inner):
                for u in range(lay.group):
                    code = meta[lay.list + row * lay.pitch + group * lay.group + u]
                    total[code & 15] += jnp.dot(
                        left[row, code >> 13], window[(code >> 4) & 511],
                        preferred_element_type=jnp.float32,
                    )
                return inner

            lax.fori_loop(0, (meta[row] + lay.group - 1) // lay.group, add_group, 0)
            for at, q in enumerate(HALF_ORDER[half]):
                stage = stages[2 * half + (1 if at < 2 else 0)]
                for j in range(per):
                    stage[at % 2, local_row, j] = total[q * per + j].astype(stage.dtype)
            for which in range(2):
                out_copy(half, local_row, which).start()
            return carry

        lax.fori_loop(0, half_rows, one_row, 0)
    for half in range(2):
        for row in range(half_rows):
            for which in range(2):
                out_copy(half, row, which).wait()


HALF_ORDER = ((0, 3, 1, 2), (0, 1, 3, 2))


def block_products(lay, lefts, windows, sizes, meta):
    slab, slots, side, _ = lefts[0].shape
    per = lay.per
    pieces = [piece.reshape(-1, side, side) for window in windows for piece in window]
    rows_in = len(windows) * sum(sizes)
    dtype = lefts[0].dtype
    any_spec = pl.BlockSpec(memory_space=pl.ANY)
    out_shape = (2, slab // 2, per, side, side)
    return pl.pallas_call(
        functools.partial(product_kernel, lay, len(lefts), sizes),
        in_specs=[pl.BlockSpec(memory_space=pltpu.SMEM)]
        + [any_spec] * (len(lefts) + len(pieces)),
        out_specs=[any_spec] * 4,
        scratch_shapes=[pltpu.VMEM(out_shape, jnp.bfloat16)] * 4
        + [
            pltpu.VMEM((slab, len(lefts) * slots, side, side), dtype),
            pltpu.VMEM((rows_in * per, side, side), dtype),
            pltpu.VMEM((slots + 1, side, side), jnp.float32),
            pltpu.SemaphoreType.DMA((len(pieces) + slab * len(lefts) + 2 * slab,)),
        ],
        out_shape=[jax.ShapeDtypeStruct(out_shape, jnp.bfloat16)] * 4,
        compiler_params=pltpu.CompilerParams(vmem_limit_bytes=VMEM_LIMIT),
        cost_estimate=pl.CostEstimate(
            flops=8_000_000_000,
            bytes_accessed=2 * (rows_in * per + 2 * slab * slots) * side * side,
            transcendentals=0,
        ),
    )(meta, *lefts, *pieces)


def met(value, flip):
    return lax.ppermute(value, "rep", [(i, i ^ flip) for i in range(lax.axis_size("rep"))])


def finish_kernel(which, branch_ref, *refs):
    sources, (kept_ref, out_ref) = refs[:6], refs[6:8]
    parts, kept, out, sems = refs[8:]
    half_rows = out.shape[1]
    loads = []
    for half in range(2):
        for i in range(3):
            source = sources[3 * half + i]
            loads.append(
                pltpu.make_async_copy(
                    source if i == 2 else source.at[0], parts.at[half, i], sems.at[half, i]
                )
            )
        rows = pl.ds(half * half_rows, half_rows)
        loads.append(
            pltpu.make_async_copy(kept_ref.at[which, rows], kept.at[half], sems.at[half, 3])
        )
    for load in loads:
        load.start()
    stores = []
    for half in range(2):
        for load in loads[4 * half : 4 * half + 4]:
            load.wait()
        for row in range(half_rows):
            squaring = branch_ref[half * half_rows + row] == 1
            total = parts[half, 0, row].astype(jnp.float32) + parts[half, 1, row].astype(jnp.float32)
            total = total + parts[half, 2, row].astype(jnp.float32)
            twice = 2.0 * kept[half, row].astype(jnp.float32)
            out[half, row] = jnp.where(squaring, total, twice - total).astype(out.dtype)
            store = pltpu.make_async_copy(
                out.at[half, row], out_ref.at[half * half_rows + row],
                sems.at[half, 4 + row],
            )
            store.start()
            stores.append(store)
    for store in stores:
        store.wait()


def finish(halves, kept, which, branch):
    _, half_rows, per, side, _ = halves[0][0].shape
    dtype = jnp.bfloat16
    any_spec = pl.BlockSpec(memory_space=pl.ANY)
    half = (half_rows, per, side, side)
    return pl.pallas_call(
        functools.partial(finish_kernel, which),
        in_specs=[pl.BlockSpec(memory_space=pltpu.SMEM)] + [any_spec] * 7,
        out_specs=any_spec,
        out_shape=jax.ShapeDtypeStruct((2 * half_rows, per, side, side), dtype),
        scratch_shapes=[
            pltpu.VMEM((2, 3) + half, dtype),
            pltpu.VMEM((2,) + half, dtype),
            pltpu.VMEM((2,) + half, dtype),
            pltpu.SemaphoreType.DMA((2, 4 + half_rows)),
        ],
        compiler_params=pltpu.CompilerParams(vmem_limit_bytes=VMEM_LIMIT),
        cost_estimate=pl.CostEstimate(flops=2_000_000_000, bytes_accessed=4 << 20, transcendentals=0),
        name="finish",
    )(branch, *halves[0], *halves[1], kept)


def pair_sum(keep, got):
    return (keep[1].astype(jnp.float32) + got[1].astype(jnp.float32)).astype(jnp.bfloat16)


def step(p_blocks, d_blocks, p_cols, d_cols, out_pcols, out_dcols, row_slot, branch):
    slab, slots, _, _ = p_blocks.shape
    per = slots // lax.axis_size("rep")
    margin = slots + 2 * SPREAD_ROWS
    reach = -(-margin // slab)
    far = margin - 2 * slab
    sizes, table = window_table(slab, margin)
    table = table * per
    window_rows = sum(sizes)

    def outer(pieces):
        part, near, rest, edge = pieces
        out1 = swapped(part, -1, 1)
        far2 = swapped(rest, 2, -2)
        near2 = swapped(near, 2, -2)
        out3 = swapped(edge, -3, 3)
        in1 = swapped(part, 1, -1)
        return part, in1, out1, near2, far2, out3

    def inner(pieces):
        return pieces + (swapped(pieces[2], 1, -1), swapped(pieces[4], 1, -1))

    p_pieces, d_pieces = packed(p_blocks, d_blocks, per, far)
    p_window = outer(p_pieces)
    d_window = outer(d_pieces)
    square_lay = Lists(slab, slots, per, 1, False)
    tangent_lay = Lists(slab, slots, per, 2, True)
    square_meta = planned(
        square_lay, reach, window_rows, ((0, 0, 0),), table, row_slot, (p_cols,), (out_pcols,)
    )
    tangent_meta = planned(
        tangent_lay, reach, window_rows, ((0, 1, 1), (1, 0, 1)), table, row_slot,
        (p_cols, d_cols), (out_pcols, out_dcols),
    )
    p_window = inner(p_window)
    d_window = inner(d_window)
    sent_a, keep_a, sent_b, keep_b = block_products(
        square_lay, (p_blocks,), (p_window,), sizes, square_meta
    )
    first_a = met(sent_a, 1)
    first_b = met(sent_b, 3)
    tsent_a, tkeep_a, tsent_b, tkeep_b = block_products(
        tangent_lay, (p_blocks, d_blocks), (p_window, d_window), sizes, tangent_meta,
    )
    tkeep_a, kept_meta = lax.optimization_barrier((tkeep_a, tangent_meta))
    kept = kept_blocks(tangent_lay, kept_meta, p_blocks, d_blocks)
    tfirst_a = met(tsent_a, 1)
    tfirst_b = met(tsent_b, 3)
    second_a = met(pair_sum(keep_a, first_a), 3)
    second_b = met(pair_sum(keep_b, first_b), 1)
    tsecond_a = met(pair_sum(tkeep_a, tfirst_a), 3)
    tsecond_b = met(pair_sum(tkeep_b, tfirst_b), 1)
    next_p = finish(
        ((keep_a, first_a, second_a), (keep_b, first_b, second_b)), kept, 0, branch
    )
    next_d = finish(
        ((tkeep_a, tfirst_a, tsecond_a), (tkeep_b, tfirst_b, tsecond_b)), kept, 1, branch
    )
    return next_p, next_d


def solution(mesh):
    return jax.shard_map(
        step,
        mesh=mesh,
        in_specs=(
            P("rows", None, None, None),
            P("rows", None, None, None),
            P(),
            P(),
            P("rows", None),
            P("rows", None),
            P(),
            P("rows"),
        ),
        out_specs=(P("rows", "rep", None, None), P("rows", "rep", None, None)),
        check_vma=False,
    )
```

```python
import functools

import jax
import jax.numpy as jnp
import numpy as np
from jax import lax
from jax.experimental import pallas as pl
from jax.experimental.pallas import tpu as pltpu
from jax.sharding import PartitionSpec as P


SPREAD_ROWS = 3
GROUPS = (16, 32)
BATCH = 2
VMEM_LIMIT = 22 << 20


def window_table(slab, margin):
    far = margin - 2 * slab
    sizes = (slab, slab, slab, slab - far, far, far, slab, far)
    own, in1, out1, near2, far2, out3, in2, in3 = np.cumsum((0,) + sizes[:-1])

    def run(start, count):
        return list(range(start, start + count))

    core0 = (
        run(out3, far) + run(near2, slab - far) + run(far2, far) + run(out1, slab)
        + run(own, slab) + run(in1, slab) + run(in2, slab) + run(in3, far)
    )
    core1 = (
        run(in3, far) + run(in2, slab) + run(in1, slab) + run(own, slab)
        + run(out1, slab) + run(far2, far) + run(near2, slab - far) + run(out3, far)
    )
    edge = [0] * (slab - far)
    return sizes, np.array(edge + core0 + edge + edge + core1 + edge, np.int32)


def swapped(value, even_step, odd_step):
    count = lax.axis_size("rows")
    pairs = [(i, (i + (odd_step if i % 2 else even_step)) % count) for i in range(count)]
    return lax.ppermute(value, "rows", pairs)


def pack_kernel(far, slab, per, *refs):
    blocks, outs, sems = refs[:2], refs[2:10], refs[10]
    core, rep = lax.axis_index("rows") % 2, lax.axis_index("rep")
    rest = slab - far
    cuts = ((core * rest, far), (0, slab), ((1 - core) * rest, far), (core * far, rest))
    copies = []
    for n, block in enumerate(blocks):
        for i, (first, rows) in enumerate(cuts):
            copies.append(
                pltpu.make_async_copy(
                    block.at[pl.ds(first, rows), pl.ds(rep * per, per)], outs[4 * n + i],
                    sems.at[n, i],
                )
            )
            copies[-1].start()
    for copy in copies:
        copy.wait()


def packed(p_blocks, d_blocks, per, far):
    slab, _, side, _ = p_blocks.shape
    dtype = p_blocks.dtype
    shapes = [(far, per), (slab, per), (far, per), (slab - far, per)] * 2
    outs = pl.pallas_call(
        functools.partial(pack_kernel, far, slab, per),
        in_specs=[pl.BlockSpec(memory_space=pltpu.HBM)] * 2,
        out_specs=[pl.BlockSpec(memory_space=pl.ANY)] * 8,
        out_shape=[jax.ShapeDtypeStruct(s + (side, side), dtype) for s in shapes],
        scratch_shapes=[pltpu.SemaphoreType.DMA((2, 4))],
        compiler_params=pltpu.CompilerParams(vmem_limit_bytes=VMEM_LIMIT),
        cost_estimate=pl.CostEstimate(flops=3_000_000_000, bytes_accessed=1 << 22, transcendentals=0),
        name="pack",
    )(*(pltpu.with_memory_space_constraint(b, pltpu.HBM) for b in (p_blocks, d_blocks)))
    return outs[:4], outs[4:]


class Lists:
    def __init__(self, slab, slots, per, n_products, kept):
        self.slab, self.slots, self.per = slab, slots, per
        self.group = GROUPS[n_products - 1]
        self.pitch = n_products * slots * per + self.group
        self.kept = slab if kept else None
        self.list = slab + (2 * slab * per if kept else 0)
        self.size = self.list + slab * self.pitch


def plan_kernel(lay, reach, window_rows, products, n, table, row_slot, *refs):
    cols, outs, meta = refs[:n], refs[n : 2 * n], refs[2 * n]
    inverse, slot_of = refs[2 * n + 1 : 3 * n + 1], refs[-1]
    slab, slots, per = lay.slab, lay.slots, lay.per
    rows = row_slot.shape[0]
    index, rep = lax.axis_index("rows"), lax.axis_index("rep")
    row_start = index * slab
    here = reach * slab
    table_base = (index % 2) * (2 * here + slab)
    span = 2 * slots + SPREAD_ROWS
    for column in range(-span, slab + span):
        for inv in inverse + ((slot_of,) if lay.kept is not None else ()):
            inv[(row_start + column + rows) & (rows - 1)] = slots
    relative = [(q ^ rep) * per for q in range(slots // per)]

    def row(s, carry):
        own = row_start + s
        for which in range(n):
            for j in range(slots):
                inverse[which][outs[which][s, j]] = relative[j // per] + j % per
        start = lay.list + s * lay.pitch
        end = start
        lefts = sorted({product[0] for product in products})
        for first in range(0, slots, BATCH):
            found = []
            for k in range(first, min(first + BATCH, slots)):
                for left in lefts:
                    stored = row_slot[cols[left][k, own]]
                    offset = (stored - row_start + here + rows) & (rows - 1)
                    code = (table[table_base + offset] << 4) + ((left * slots + k) << 13)
                    for which_left, right, out in products:
                        if which_left != left:
                            continue
                        base = right * window_rows * per if n > 1 else 0
                        for m in range(per):
                            target = inverse[out][cols[right][rep * per + m, stored]]
                            found.append((target, code + ((base + m) << 4)))
            for target, entry in found:
                meta[end] = entry + target
                end += jnp.where(target < slots, 1, 0)
        for u in range(lay.group):
            meta[end + u] = slots
        meta[s] = end - start
        if lay.kept is not None:
            for which in range(n):
                for k in range(slots):
                    slot_of[cols[which][k, own]] = k
                for j in range(per):
                    at = lay.kept + (which * slab + s) * per + j
                    meta[at] = slot_of[outs[which][s, rep * per + j]]
                for k in range(slots):
                    slot_of[cols[which][k, own]] = slots
        for which in range(n):
            for j in range(slots):
                inverse[which][outs[which][s, j]] = slots
        return carry

    lax.fori_loop(0, slab, row, 0)


def planned(lay, reach, window_rows, products, table, row_slot, cols, outs):
    n = len(cols)
    rows = row_slot.shape[0]
    smem = pl.BlockSpec(memory_space=pltpu.SMEM)
    return pl.pallas_call(
        functools.partial(plan_kernel, lay, reach, window_rows, products, n),
        in_specs=[smem] * (2 + 2 * n),
        out_specs=smem,
        out_shape=jax.ShapeDtypeStruct((lay.size,), jnp.int32),
        scratch_shapes=[pltpu.SMEM((rows,), jnp.int32)] * (n + 1),
        compiler_params=pltpu.CompilerParams(vmem_limit_bytes=VMEM_LIMIT),
        cost_estimate=pl.CostEstimate(flops=4_000_000_000, bytes_accessed=65536, transcendentals=0),
        name="plan",
    )(jnp.asarray(table), row_slot, *(ids.T for ids in cols), *outs)


def kept_kernel(lay, meta, p_ref, d_ref, out_ref, held, sems, out_sem):
    slab, slots, per = lay.slab, lay.slots, lay.per
    loads = []
    for which, blocks in enumerate((p_ref, d_ref)):
        for s in range(slab):
            for j in range(per):
                n = (which * slab + s) * per + j
                k = meta[lay.kept + n]
                load = pltpu.make_async_copy(
                    blocks.at[s, jnp.minimum(k, slots - 1)], held.at[which, s, j], sems.at[n]
                )
                load.start()
                loads.append((load, k, which, s, j))
    for load, k, which, s, j in loads:
        load.wait()

        @pl.when(k == slots)
        def _():
            held[which, s, j] = jnp.zeros(held.shape[3:], held.dtype)

    store = pltpu.make_async_copy(held, out_ref, out_sem)
    store.start()
    store.wait()


def kept_blocks(lay, meta, p_blocks, d_blocks):
    slab, _, side, _ = p_blocks.shape
    shape = (2, slab, lay.per, side, side)
    return pl.pallas_call(
        functools.partial(kept_kernel, lay),
        in_specs=[pl.BlockSpec(memory_space=pltpu.SMEM)] + [pl.BlockSpec(memory_space=pl.ANY)] * 2,
        out_specs=pl.BlockSpec(memory_space=pl.ANY),
        out_shape=jax.ShapeDtypeStruct(shape, p_blocks.dtype),
        scratch_shapes=[
            pltpu.VMEM(shape, p_blocks.dtype),
            pltpu.SemaphoreType.DMA((2 * slab * lay.per,)),
            pltpu.SemaphoreType.DMA,
        ],
        compiler_params=pltpu.CompilerParams(vmem_limit_bytes=VMEM_LIMIT),
        cost_estimate=pl.CostEstimate(flops=3_000_000_000, bytes_accessed=1 << 21, transcendentals=0),
        name="kept",
    )(meta, p_blocks, d_blocks)


def product_kernel(lay, n_left, sizes, meta, *refs):
    left_refs = refs[:n_left]
    pieces = refs[n_left : n_left + n_left * len(sizes)]
    outs, stages = refs[-12:-8], refs[-8:-4]
    left, window, total, sems = refs[-4:]
    slab, slots, per = lay.slab, lay.slots, lay.per
    half_rows = slab // 2
    window_sem, left_sem, out_sem = 0, len(pieces), len(pieces) + slab * n_left

    def left_copy(row, n):
        return pltpu.make_async_copy(
            left_refs[n].at[row], left.at[row, pl.ds(n * slots, slots)],
            sems.at[left_sem + row * n_left + n],
        )

    copies, base = [], 0
    for index, piece in enumerate(pieces):
        size = sizes[index % len(sizes)]
        copies.append(
            pltpu.make_async_copy(
                piece, window.at[pl.ds(base * per, size * per)], sems.at[window_sem + index]
            )
        )
        base += size
    for copy in copies:
        copy.start()
    for row in range(slab):
        for n in range(n_left):
            left_copy(row, n).start()
    for copy in copies:
        copy.wait()

    def out_copy(half, row, which):
        number = 2 * half + which
        return pltpu.make_async_copy(
            stages[number].at[:, row], outs[number].at[:, row],
            sems.at[out_sem + (half * half_rows + row) * 2 + which],
        )

    for half in range(2):

        def one_row(local_row, carry):
            row = half * half_rows + local_row
            for n in range(n_left):
                left_copy(row, n).wait()
            total[...] = jnp.zeros_like(total)

            def add_group(group, inner):
                for u in range(lay.group):
                    code = meta[lay.list + row * lay.pitch + group * lay.group + u]
                    total[code & 15] += jnp.dot(
                        left[row, code >> 13], window[(code >> 4) & 511],
                        preferred_element_type=jnp.float32,
                    )
                return inner

            lax.fori_loop(0, (meta[row] + lay.group - 1) // lay.group, add_group, 0)
            for at, q in enumerate(HALF_ORDER[half]):
                stage = stages[2 * half + (1 if at < 2 else 0)]
                for j in range(per):
                    stage[at % 2, local_row, j] = total[q * per + j].astype(stage.dtype)
            for which in range(2):
                out_copy(half, local_row, which).start()
            return carry

        lax.fori_loop(0, half_rows, one_row, 0)
    for half in range(2):
        for row in range(half_rows):
            for which in range(2):
                out_copy(half, row, which).wait()


HALF_ORDER = ((0, 3, 1, 2), (0, 1, 3, 2))


def block_products(lay, lefts, windows, sizes, meta):
    slab, slots, side, _ = lefts[0].shape
    per = lay.per
    pieces = [piece.reshape(-1, side, side) for window in windows for piece in window]
    rows_in = len(windows) * sum(sizes)
    dtype = lefts[0].dtype
    any_spec = pl.BlockSpec(memory_space=pl.ANY)
    out_shape = (2, slab // 2, per, side, side)
    return pl.pallas_call(
        functools.partial(product_kernel, lay, len(lefts), sizes),
        in_specs=[pl.BlockSpec(memory_space=pltpu.SMEM)]
        + [any_spec] * (len(lefts) + len(pieces)),
        out_specs=[any_spec] * 4,
        scratch_shapes=[pltpu.VMEM(out_shape, jnp.bfloat16)] * 4
        + [
            pltpu.VMEM((slab, len(lefts) * slots, side, side), dtype),
            pltpu.VMEM((rows_in * per, side, side), dtype),
            pltpu.VMEM((slots + 1, side, side), jnp.float32),
            pltpu.SemaphoreType.DMA((len(pieces) + slab * len(lefts) + 2 * slab,)),
        ],
        out_shape=[jax.ShapeDtypeStruct(out_shape, jnp.bfloat16)] * 4,
        compiler_params=pltpu.CompilerParams(vmem_limit_bytes=VMEM_LIMIT),
        cost_estimate=pl.CostEstimate(
            flops=8_000_000_000,
            bytes_accessed=2 * (rows_in * per + 2 * slab * slots) * side * side,
            transcendentals=0,
        ),
    )(meta, *lefts, *pieces)


def met(value, flip):
    return lax.ppermute(value, "rep", [(i, i ^ flip) for i in range(lax.axis_size("rep"))])


def finish_kernel(which, branch_ref, *refs):
    sources, (kept_ref, out_ref) = refs[:6], refs[6:8]
    parts, kept, out, sems = refs[8:]
    half_rows = out.shape[1]
    loads = []
    for half in range(2):
        for i in range(3):
            source = sources[3 * half + i]
            loads.append(
                pltpu.make_async_copy(
                    source if i == 2 else source.at[0], parts.at[half, i], sems.at[half, i]
                )
            )
        rows = pl.ds(half * half_rows, half_rows)
        loads.append(
            pltpu.make_async_copy(kept_ref.at[which, rows], kept.at[half], sems.at[half, 3])
        )
    for load in loads:
        load.start()
    stores = []
    for half in range(2):
        for load in loads[4 * half : 4 * half + 4]:
            load.wait()
        for row in range(half_rows):
            squaring = branch_ref[half * half_rows + row] == 1
            total = parts[half, 0, row].astype(jnp.float32) + parts[half, 1, row].astype(jnp.float32)
            total = total + parts[half, 2, row].astype(jnp.float32)
            twice = 2.0 * kept[half, row].astype(jnp.float32)
            out[half, row] = jnp.where(squaring, total, twice - total).astype(out.dtype)
            store = pltpu.make_async_copy(
                out.at[half, row], out_ref.at[half * half_rows + row],
                sems.at[half, 4 + row],
            )
            store.start()
            stores.append(store)
    for store in stores:
        store.wait()


def finish(halves, kept, which, branch):
    _, half_rows, per, side, _ = halves[0][0].shape
    dtype = jnp.bfloat16
    any_spec = pl.BlockSpec(memory_space=pl.ANY)
    half = (half_rows, per, side, side)
    return pl.pallas_call(
        functools.partial(finish_kernel, which),
        in_specs=[pl.BlockSpec(memory_space=pltpu.SMEM)] + [any_spec] * 7,
        out_specs=any_spec,
        out_shape=jax.ShapeDtypeStruct((2 * half_rows, per, side, side), dtype),
        scratch_shapes=[
            pltpu.VMEM((2, 3) + half, dtype),
            pltpu.VMEM((2,) + half, dtype),
            pltpu.VMEM((2,) + half, dtype),
            pltpu.SemaphoreType.DMA((2, 4 + half_rows)),
        ],
        compiler_params=pltpu.CompilerParams(vmem_limit_bytes=VMEM_LIMIT),
        cost_estimate=pl.CostEstimate(flops=2_000_000_000, bytes_accessed=4 << 20, transcendentals=0),
        name="finish",
    )(branch, *halves[0], *halves[1], kept)


def pair_sum(keep, got):
    return (keep[1].astype(jnp.float32) + got[1].astype(jnp.float32)).astype(jnp.bfloat16)


def step(p_blocks, d_blocks, p_cols, d_cols, out_pcols, out_dcols, row_slot, branch):
    slab, slots, _, _ = p_blocks.shape
    per = slots // lax.axis_size("rep")
    margin = slots + 2 * SPREAD_ROWS
    reach = -(-margin // slab)
    far = margin - 2 * slab
    sizes, table = window_table(slab, margin)
    table = table * per
    window_rows = sum(sizes)

    def outer(pieces):
        edge, part, rest, near = pieces
        out1 = swapped(part, -1, 1)
        far2 = swapped(rest, 2, -2)
        near2 = swapped(near, 2, -2)
        out3 = swapped(edge, -3, 3)
        in1 = swapped(part, 1, -1)
        return part, in1, out1, near2, far2, out3

    def inner(pieces):
        return pieces + (swapped(pieces[2], 1, -1), swapped(pieces[4], 1, -1))

    p_pieces, d_pieces = packed(p_blocks, d_blocks, per, far)
    p_window = outer(p_pieces)
    d_window = outer(d_pieces)
    square_lay = Lists(slab, slots, per, 1, False)
    tangent_lay = Lists(slab, slots, per, 2, True)
    square_meta = planned(
        square_lay, reach, window_rows, ((0, 0, 0),), table, row_slot, (p_cols,), (out_pcols,)
    )
    tangent_meta = planned(
        tangent_lay, reach, window_rows, ((0, 1, 1), (1, 0, 1)), table, row_slot,
        (p_cols, d_cols), (out_pcols, out_dcols),
    )
    p_window = inner(p_window)
    d_window = inner(d_window)
    sent_a, keep_a, sent_b, keep_b = block_products(
        square_lay, (p_blocks,), (p_window,), sizes, square_meta
    )
    first_a = met(sent_a, 1)
    first_b = met(sent_b, 3)
    tsent_a, tkeep_a, tsent_b, tkeep_b = block_products(
        tangent_lay, (p_blocks, d_blocks), (p_window, d_window), sizes, tangent_meta,
    )
    tkeep_a, kept_meta = lax.optimization_barrier((tkeep_a, tangent_meta))
    kept = kept_blocks(tangent_lay, kept_meta, p_blocks, d_blocks)
    tfirst_a = met(tsent_a, 1)
    tfirst_b = met(tsent_b, 3)
    second_a = met(pair_sum(keep_a, first_a), 3)
    second_b = met(pair_sum(keep_b, first_b), 1)
    tsecond_a = met(pair_sum(tkeep_a, tfirst_a), 3)
    tsecond_b = met(pair_sum(tkeep_b, tfirst_b), 1)
    next_p = finish(
        ((keep_a, first_a, second_a), (keep_b, first_b, second_b)), kept, 0, branch
    )
    next_d = finish(
        ((tkeep_a, tfirst_a, tsecond_a), (tkeep_b, tfirst_b, tsecond_b)), kept, 1, branch
    )
    return next_p, next_d


def solution(mesh):
    return jax.shard_map(
        step,
        mesh=mesh,
        in_specs=(
            P("rows", None, None, None),
            P("rows", None, None, None),
            P(),
            P(),
            P("rows", None),
            P("rows", None),
            P(),
            P("rows"),
        ),
        out_specs=(P("rows", "rep", None, None), P("rows", "rep", None, None)),
        check_vma=False,
    )
```

```python
import functools

import jax
import jax.numpy as jnp
import numpy as np
from jax import lax
from jax.experimental import pallas as pl
from jax.experimental.pallas import tpu as pltpu
from jax.sharding import PartitionSpec as P


SPREAD_ROWS = 3
GROUPS = (16, 32)
BATCH = 2
VMEM_LIMIT = 22 << 20


def window_table(slab, margin):
    far = margin - 2 * slab
    sizes = (slab, slab, slab, slab - far, far, far, slab, far)
    own, in1, out1, near2, far2, out3, in2, in3 = np.cumsum((0,) + sizes[:-1])

    def run(start, count):
        return list(range(start, start + count))

    core0 = (
        run(out3, far) + run(near2, slab - far) + run(far2, far) + run(out1, slab)
        + run(own, slab) + run(in1, slab) + run(in2, slab) + run(in3, far)
    )
    core1 = (
        run(in3, far) + run(in2, slab) + run(in1, slab) + run(own, slab)
        + run(out1, slab) + run(far2, far) + run(near2, slab - far) + run(out3, far)
    )
    edge = [0] * (slab - far)
    return sizes, np.array(edge + core0 + edge + edge + core1 + edge, np.int32)


def swapped(value, even_step, odd_step):
    count = lax.axis_size("rows")
    pairs = [(i, (i + (odd_step if i % 2 else even_step)) % count) for i in range(count)]
    return lax.ppermute(value, "rows", pairs)


def pack_kernel(far, slab, per, *refs):
    blocks, outs, sems = refs[:2], refs[2:10], refs[10]
    core, rep = lax.axis_index("rows") % 2, lax.axis_index("rep")
    rest = slab - far
    cuts = ((core * rest, far), (0, slab), ((1 - core) * rest, far), (core * far, rest))
    copies = []
    for n, block in enumerate(blocks):
        for i, (first, rows) in enumerate(cuts):
            copies.append(
                pltpu.make_async_copy(
                    block.at[pl.ds(first, rows), pl.ds(rep * per, per)], outs[4 * n + i],
                    sems.at[n, i],
                )
            )
            copies[-1].start()
    for copy in copies:
        copy.wait()


def packed(p_blocks, d_blocks, per, far):
    slab, _, side, _ = p_blocks.shape
    dtype = p_blocks.dtype
    shapes = [(far, per), (slab, per), (far, per), (slab - far, per)] * 2
    outs = pl.pallas_call(
        functools.partial(pack_kernel, far, slab, per),
        in_specs=[pl.BlockSpec(memory_space=pltpu.HBM)] * 2,
        out_specs=[pl.BlockSpec(memory_space=pl.ANY)] * 8,
        out_shape=[jax.ShapeDtypeStruct(s + (side, side), dtype) for s in shapes],
        scratch_shapes=[pltpu.SemaphoreType.DMA((2, 4))],
        compiler_params=pltpu.CompilerParams(vmem_limit_bytes=VMEM_LIMIT),
        cost_estimate=pl.CostEstimate(flops=3_000_000_000, bytes_accessed=1 << 22, transcendentals=0),
        name="pack",
    )(*(pltpu.with_memory_space_constraint(b, pltpu.HBM) for b in (p_blocks, d_blocks)))
    return outs[:4], outs[4:]


class Lists:
    def __init__(self, slab, slots, per, n_products, kept):
        self.slab, self.slots, self.per = slab, slots, per
        self.group = GROUPS[n_products - 1]
        self.pitch = n_products * slots * per + self.group
        self.kept = slab if kept else None
        self.list = slab + (2 * slab * per if kept else 0)
        self.size = self.list + slab * self.pitch


def plan_kernel(lay, reach, window_rows, products, n, table, row_slot, *refs):
    cols, outs, meta = refs[:n], refs[n : 2 * n], refs[2 * n]
    inverse, slot_of = refs[2 * n + 1 : 3 * n + 1], refs[-1]
    slab, slots, per = lay.slab, lay.slots, lay.per
    rows = row_slot.shape[0]
    index, rep = lax.axis_index("rows"), lax.axis_index("rep")
    row_start = index * slab
    here = reach * slab
    table_base = (index % 2) * (2 * here + slab)
    span = 2 * slots + SPREAD_ROWS
    for column in range(-span, slab + span):
        for inv in inverse + ((slot_of,) if lay.kept is not None else ()):
            inv[(row_start + column + rows) & (rows - 1)] = slots
    relative = [(q ^ rep) * per for q in range(slots // per)]

    def row(s, carry):
        own = row_start + s
        for which in range(n):
            for j in range(slots):
                inverse[which][outs[which][s, j]] = relative[j // per] + j % per
        start = lay.list + s * lay.pitch
        end = start
        lefts = sorted({product[0] for product in products})
        for first in range(0, slots, BATCH):
            found = []
            for k in range(first, min(first + BATCH, slots)):
                for left in lefts:
                    stored = row_slot[cols[left][k, own]]
                    offset = (stored - row_start + here + rows) & (rows - 1)
                    code = (table[table_base + offset] << 4) + ((left * slots + k) << 13)
                    for which_left, right, out in products:
                        if which_left != left:
                            continue
                        base = right * window_rows * per if n > 1 else 0
                        for m in range(per):
                            target = inverse[out][cols[right][rep * per + m, stored]]
                            found.append((target, code + ((base + m) << 4)))
            for target, entry in found:
                meta[end] = entry + target
                end += jnp.where(target < slots, 1, 0)
        for u in range(lay.group):
            meta[end + u] = slots
        meta[s] = end - start
        if lay.kept is not None:
            for which in range(n):
                for k in range(slots):
                    slot_of[cols[which][k, own]] = k
                for j in range(per):
                    at = lay.kept + (which * slab + s) * per + j
                    meta[at] = slot_of[outs[which][s, rep * per + j]]
                for k in range(slots):
                    slot_of[cols[which][k, own]] = slots
        for which in range(n):
            for j in range(slots):
                inverse[which][outs[which][s, j]] = slots
        return carry

    lax.fori_loop(0, slab, row, 0)


def planned(lay, reach, window_rows, products, table, row_slot, cols, outs):
    n = len(cols)
    rows = row_slot.shape[0]
    smem = pl.BlockSpec(memory_space=pltpu.SMEM)
    return pl.pallas_call(
        functools.partial(plan_kernel, lay, reach, window_rows, products, n),
        in_specs=[smem] * (2 + 2 * n),
        out_specs=smem,
        out_shape=jax.ShapeDtypeStruct((lay.size,), jnp.int32),
        scratch_shapes=[pltpu.SMEM((rows,), jnp.int32)] * (n + 1),
        compiler_params=pltpu.CompilerParams(vmem_limit_bytes=VMEM_LIMIT),
        cost_estimate=pl.CostEstimate(flops=4_000_000_000, bytes_accessed=65536, transcendentals=0),
        name="plan",
    )(jnp.asarray(table), row_slot, *(ids.T for ids in cols), *outs)


def kept_kernel(lay, meta, p_ref, d_ref, out_ref, held, sems, out_sem):
    slab, slots, per = lay.slab, lay.slots, lay.per
    loads = []
    for which, blocks in enumerate((p_ref, d_ref)):
        for s in range(slab):
            for j in range(per):
                n = (which * slab + s) * per + j
                k = meta[lay.kept + n]
                load = pltpu.make_async_copy(
                    blocks.at[s, jnp.minimum(k, slots - 1)], held.at[which, s, j], sems.at[n]
                )
                load.start()
                loads.append((load, k, which, s, j))
    for load, k, which, s, j in loads:
        load.wait()

        @pl.when(k == slots)
        def _():
            held[which, s, j] = jnp.zeros(held.shape[3:], held.dtype)

    store = pltpu.make_async_copy(held, out_ref, out_sem)
    store.start()
    store.wait()


def kept_blocks(lay, meta, p_blocks, d_blocks):
    slab, _, side, _ = p_blocks.shape
    shape = (2, slab, lay.per, side, side)
    return pl.pallas_call(
        functools.partial(kept_kernel, lay),
        in_specs=[pl.BlockSpec(memory_space=pltpu.SMEM)] + [pl.BlockSpec(memory_space=pl.ANY)] * 2,
        out_specs=pl.BlockSpec(memory_space=pl.ANY),
        out_shape=jax.ShapeDtypeStruct(shape, p_blocks.dtype),
        scratch_shapes=[
            pltpu.VMEM(shape, p_blocks.dtype),
            pltpu.SemaphoreType.DMA((2 * slab * lay.per,)),
            pltpu.SemaphoreType.DMA,
        ],
        compiler_params=pltpu.CompilerParams(vmem_limit_bytes=VMEM_LIMIT),
        cost_estimate=pl.CostEstimate(flops=3_000_000_000, bytes_accessed=1 << 21, transcendentals=0),
        name="kept",
    )(meta, p_blocks, d_blocks)


def product_kernel(lay, n_left, sizes, meta, *refs):
    left_refs = refs[:n_left]
    pieces = refs[n_left : n_left + n_left * len(sizes)]
    outs, (window, total) = refs[-6:-2], refs[-2:]
    slab, slots, per = lay.slab, lay.slots, lay.per
    half_rows = slab // 2

    base = 0
    for index, piece in enumerate(pieces):
        size = sizes[index % len(sizes)]

        def move(row, carry, piece=piece, base=base):
            window[pl.ds((base + row) * per, per)] = piece[row]
            return carry

        lax.fori_loop(0, size, move, 0)
        base += size

    for half in range(2):

        def one_row(local_row, carry):
            row = half * half_rows + local_row
            total[...] = jnp.zeros_like(total)

            def add_group(group, inner):
                for u in range(lay.group):
                    code = meta[lay.list + row * lay.pitch + group * lay.group + u]
                    k = code >> 13
                    if n_left == 1:
                        left = left_refs[0][row, k]
                    else:
                        second = k >= slots
                        k = jnp.where(second, k - slots, k)
                        left = jnp.where(second, left_refs[1][row, k], left_refs[0][row, k])
                    total[code & 15] += jnp.dot(
                        left, window[(code >> 4) & 511], preferred_element_type=jnp.float32
                    )
                return inner

            lax.fori_loop(0, (meta[row] + lay.group - 1) // lay.group, add_group, 0)
            for at, q in enumerate(HALF_ORDER[half]):
                out = outs[2 * half + (1 if at < 2 else 0)]
                for j in range(per):
                    out[at % 2, local_row, j] = total[q * per + j].astype(out.dtype)
            return carry

        lax.fori_loop(0, half_rows, one_row, 0)


HALF_ORDER = ((0, 3, 1, 2), (0, 1, 3, 2))


def block_products(lay, lefts, windows, sizes, meta):
    slab, slots, side, _ = lefts[0].shape
    per = lay.per
    pieces = [piece for window in windows for piece in window]
    rows_in = len(windows) * sum(sizes)
    vmem = pl.BlockSpec(memory_space=pltpu.VMEM)
    out_shape = (2, slab // 2, per, side, side)
    return pl.pallas_call(
        functools.partial(product_kernel, lay, len(lefts), sizes),
        in_specs=[pl.BlockSpec(memory_space=pltpu.SMEM)] + [vmem] * (len(lefts) + len(pieces)),
        out_specs=[vmem] * 4,
        scratch_shapes=[
            pltpu.VMEM((rows_in * per, side, side), lefts[0].dtype),
            pltpu.VMEM((slots + 1, side, side), jnp.float32),
        ],
        out_shape=[jax.ShapeDtypeStruct(out_shape, jnp.bfloat16)] * 4,
        compiler_params=pltpu.CompilerParams(vmem_limit_bytes=VMEM_LIMIT),
        cost_estimate=pl.CostEstimate(
            flops=8_000_000_000,
            bytes_accessed=2 * (rows_in * per + 2 * slab * slots) * side * side,
            transcendentals=0,
        ),
    )(meta, *lefts, *pieces)


def met(value, flip):
    return lax.ppermute(value, "rep", [(i, i ^ flip) for i in range(lax.axis_size("rep"))])


def finish_kernel(which, branch_ref, *refs):
    sources, (kept_ref, out_ref) = refs[:6], refs[6:]
    half_rows = sources[2].shape[0]
    for half in range(2):
        keep, first, second = sources[3 * half : 3 * half + 3]
        for local_row in range(half_rows):
            row = half * half_rows + local_row
            squaring = branch_ref[row] == 1
            total = keep[0, local_row].astype(jnp.float32) + first[0, local_row].astype(jnp.float32)
            total = total + second[local_row].astype(jnp.float32)
            twice = 2.0 * kept_ref[which, row].astype(jnp.float32)
            out_ref[row] = jnp.where(squaring, total, twice - total).astype(out_ref.dtype)


def finish(halves, kept, which, branch):
    _, half_rows, per, side, _ = halves[0][0].shape
    vmem = pl.BlockSpec(memory_space=pltpu.VMEM)
    return pl.pallas_call(
        functools.partial(finish_kernel, which),
        in_specs=[pl.BlockSpec(memory_space=pltpu.SMEM)] + [vmem] * 7,
        out_specs=vmem,
        out_shape=jax.ShapeDtypeStruct((2 * half_rows, per, side, side), jnp.bfloat16),
        compiler_params=pltpu.CompilerParams(vmem_limit_bytes=VMEM_LIMIT),
        cost_estimate=pl.CostEstimate(flops=2_000_000_000, bytes_accessed=4 << 20, transcendentals=0),
        name="finish",
    )(branch, *halves[0], *halves[1], kept)


def pair_sum(keep, got):
    return (keep[1].astype(jnp.float32) + got[1].astype(jnp.float32)).astype(jnp.bfloat16)


def step(p_blocks, d_blocks, p_cols, d_cols, out_pcols, out_dcols, row_slot, branch):
    slab, slots, _, _ = p_blocks.shape
    per = slots // lax.axis_size("rep")
    margin = slots + 2 * SPREAD_ROWS
    reach = -(-margin // slab)
    far = margin - 2 * slab
    sizes, table = window_table(slab, margin)
    table = table * per
    window_rows = sum(sizes)

    def outer(pieces):
        edge, part, rest, near = pieces
        out1 = swapped(part, -1, 1)
        far2 = swapped(rest, 2, -2)
        near2 = swapped(near, 2, -2)
        out3 = swapped(edge, -3, 3)
        in1 = swapped(part, 1, -1)
        return part, in1, out1, near2, far2, out3

    def inner(pieces):
        return pieces + (swapped(pieces[2], 1, -1), swapped(pieces[4], 1, -1))

    p_pieces, d_pieces = packed(p_blocks, d_blocks, per, far)
    p_window = outer(p_pieces)
    d_window = outer(d_pieces)
    square_lay = Lists(slab, slots, per, 1, False)
    tangent_lay = Lists(slab, slots, per, 2, True)
    square_meta = planned(
        square_lay, reach, window_rows, ((0, 0, 0),), table, row_slot, (p_cols,), (out_pcols,)
    )
    p_window = inner(p_window)
    d_window = inner(d_window)
    sent_a, keep_a, sent_b, keep_b = block_products(
        square_lay, (p_blocks,), (p_window,), sizes, square_meta
    )
    first_a = met(sent_a, 1)
    first_b = met(sent_b, 3)
    keep_a, later_slot = lax.optimization_barrier((keep_a, row_slot))
    tangent_meta = planned(
        tangent_lay, reach, window_rows, ((0, 1, 1), (1, 0, 1)), table, later_slot,
        (p_cols, d_cols), (out_pcols, out_dcols),
    )
    tsent_a, tkeep_a, tsent_b, tkeep_b = block_products(
        tangent_lay, (p_blocks, d_blocks), (p_window, d_window), sizes, tangent_meta,
    )
    tkeep_a, kept_meta = lax.optimization_barrier((tkeep_a, tangent_meta))
    kept = kept_blocks(tangent_lay, kept_meta, p_blocks, d_blocks)
    tfirst_a = met(tsent_a, 1)
    tfirst_b = met(tsent_b, 3)
    second_a = met(pair_sum(keep_a, first_a), 3)
    second_b = met(pair_sum(keep_b, first_b), 1)
    tsecond_a = met(pair_sum(tkeep_a, tfirst_a), 3)
    tsecond_b = met(pair_sum(tkeep_b, tfirst_b), 1)
    next_p = finish(
        ((keep_a, first_a, second_a), (keep_b, first_b, second_b)), kept, 0, branch
    )
    next_d = finish(
        ((tkeep_a, tfirst_a, tsecond_a), (tkeep_b, tfirst_b, tsecond_b)), kept, 1, branch
    )
    return next_p, next_d


def solution(mesh):
    return jax.shard_map(
        step,
        mesh=mesh,
        in_specs=(
            P("rows", None, None, None),
            P("rows", None, None, None),
            P(),
            P(),
            P("rows", None),
            P("rows", None),
            P(),
            P("rows"),
        ),
        out_specs=(P("rows", "rep", None, None), P("rows", "rep", None, None)),
        check_vma=False,
    )
```
